768 devices in a mesh: grp: 48 (over z, x), row: 16 (over y, core).
Axes of the slice: x: 4, y: 8, z: 12, core: 2. Of those that a mesh axis runs over, the one named last changes fastest.
Arguments:
- gll_state: float32 [8, 32, 16, 98304], P(None, None, None, ('grp', 'row')), may hold values from -6 to 6
- metric: float32 [16, 98304], P(None, ('grp', 'row')), may hold values from 0.7 to 1.4
- phys_owner: int32 [98304, 4, 1], P(('grp', 'row')), may hold values from 0 to 47; in each aligned block of 512 rows (0 to 511, 512 to 1023, ..., all dimensions but the last counted through in order) at most 22 rows name the same one
- neighbours: int32 [4, 98304], P(None, ('grp', 'row')), may hold values from 0 to 98303, as said below
- phys_rate: float32 [32, 811008], P(None, ('grp', 'row')), may hold values from 0.2 to 2
- phys_forcing: float32 [32, 811008], P(None, ('grp', 'row')), may hold values from -6 to 6
- field_mix: float32 [8, 8], replicated, may hold values from -2 to 2
Outputs:
- gll_tend: float32 [8, 32, 16, 98304], P(None, None, None, ('grp', 'row'))
The draws below stay inside these ranges and needn't reach their ends.
Inputs may be any that keep to these rules, and one draw needn't show every extreme that they name: `phys_owner`: in the 512 rows of one device, no owner is named more than 22 times, and some owner reaches 22. `neighbours`: rows 0 and 1 of element e are e - 1 and e + 1, cyclically over 98304 elements; rows 2 and 3 lie 2 to 32 positions before and after e, cyclically, and some element has a neighbour exactly 32 positions away.
All inputs are finite; a program needn't handle non-finite values.
Results may differ from the reference program's by a relative error of at most 0.000094.
Values sent between devices are 32-bit elements; how exact they have to be, the bound alone decides.
A program may use at most 32 MiB of HBM per device.

```python
import math
import jax
import jax.numpy as jnp
import numpy as np
from jax import lax

NF = 8
NLEV = 32
NODES = 16
E_DEV = 128
HALO = 32
CAP = 22
ELEMS = 98304
SLOTS = 811008
N_GRP = 48
N_ROW = 16


def draw_neighbours(key, part):
    first_key = jax.random.fold_in(key, 11)
    second_key = jax.random.fold_in(key, 23)
    elem_ids = jnp.arange(ELEMS, dtype=jnp.int32)
    south_step = jax.random.randint(first_key, (ELEMS,), 2, HALO + 1, dtype=jnp.int32)
    north_step = jax.random.randint(second_key, (ELEMS,), 2, HALO + 1, dtype=jnp.int32)
    north_step = jnp.where(elem_ids == 0, HALO, north_step)
    return jnp.stack([(elem_ids - 1) % ELEMS, (elem_ids + 1) % ELEMS, (elem_ids - south_step) % ELEMS, (elem_ids + north_step) % ELEMS]).astype(jnp.int32)


def shard_levels(own_key, dims, shards, smallest, top_value):
    def one(dim, blocks):
        heights = jax.random.uniform(jax.random.fold_in(jax.random.fold_in(own_key, 6), dim), (blocks,), jnp.float32, smallest / len(shards), top_value / len(shards))
        return jnp.repeat(jnp.exp(heights), dims[dim] // blocks).reshape((-1,) + (1,) * (len(dims) - dim - 1))

    gain = one(*shards[0])
    for cut in shards[1:]:
        gain = gain * one(*cut)
    return gain


def routed_block(stream_key, own, number, rows, number_of, top, most, lean):
    sequence = jax.random.permutation(stream_key, number_of)
    crowded, usual = portions_of(number_of, rows * top, most, lean, True), portions_of(number_of, rows * top, most, lean, False)
    places = jnp.arange(number_of)

    def named(tallies, turn):
        used = int((tallies > 0).sum())
        fixed = max(1, used // 4)
        moved = fixed + (places - fixed + turn * (used - fixed)) % max(1, number_of - fixed)
        return jnp.zeros((number_of,), jnp.int32).at[sequence[jnp.where(places < fixed, places, moved)]].set(jnp.asarray(tallies, jnp.int32))

    tallies = jnp.where(number % 4 == 0, named(crowded, number // 4), named(usual, number - number // 4 - 1))
    mixed = jax.random.permutation(jax.random.fold_in(own, 3), number_of)
    donor, sink = mixed[0:number_of // 2 * 2:2], mixed[1:number_of // 2 * 2:2]
    margin = jnp.minimum(tallies[donor] - 1, most - tallies[sink]) // 2
    margin = jnp.where((donor == sequence[0]) | (sink == sequence[0]) | (tallies[sink] == 0), 0, jnp.maximum(margin, 0))
    moved = jax.random.randint(jax.random.fold_in(own, 4), (number_of // 2,), 0, 1 << 20) % (margin + 1)
    tallies = tallies.at[donor].add(-moved).at[sink].add(moved)
    labels = jnp.searchsorted(jnp.cumsum(tallies), jnp.arange(rows * top), side="right").astype(jnp.int32)
    table = labels.reshape(top, rows).T
    table = table[jax.random.permutation(jax.random.fold_in(own, 1), rows)]
    turn = jax.random.randint(jax.random.fold_in(own, 2), (rows, 1), 0, top)
    return jnp.take_along_axis(table, (jnp.arange(top)[None, :] + turn) % top, axis=1)


def portions_of(amount, total, bound, lean, full):
    portions = [(1 << 20) // math.isqrt(grade ** lean) + 1 for grade in range(1, amount + 1)]
    largest = bound if full else min(bound, max(-(-total // amount), total * portions[0] // sum(portions)))
    least = 1 if total - largest >= amount - 1 else 0
    counts, rest = [largest] + [least] * (amount - 1), total - largest - least * (amount - 1)
    while rest > 0:
        free = [i for i in range(1, amount) if counts[i] < largest] or [i for i in range(1, amount) if counts[i] < bound]
        mass, left = sum([portions[i] for i in free]), rest
        for i in free:
            more = min(bound - counts[i], max(1, left * portions[i] // mass), rest)
            counts[i] = counts[i] + more
            rest = rest - more
    return np.array(counts)


def centred(stream_key, extent, width, limit, split=(), kind=jnp.bfloat16):
    loudness = shard_levels(stream_key, extent, split, -0.22, 0.18) if split else 1.0
    values = jax.random.normal(stream_key, extent, jnp.float32) * width * loudness
    return jnp.minimum(jnp.maximum(values, -limit), limit).astype(kind)


def setup_inputs(seed: int = 0) -> dict:
    streams_of = jax.random.split(jax.random.key(seed), 8)
    gll_state = centred(streams_of[0], (NF, NLEV, NODES, ELEMS), 1.0, 6.0, ((3, 768),), jnp.float32)
    metric = jnp.clip(jnp.exp(math.log(1.4) - 0.6931472 * jax.random.uniform(streams_of[1], (NODES, ELEMS), jnp.float32) ** shard_levels(streams_of[1], (NODES, ELEMS), ((1, 768),), -0.2, 0.2)), 0.7, 1.4)
    phys_owner_keys = jax.random.split(jax.random.fold_in(streams_of[2], 1), ELEMS * 4 // (4 * E_DEV))
    phys_owner_turns = jax.random.permutation(jax.random.fold_in(streams_of[2], 3), ELEMS * 4 // (4 * E_DEV))
    phys_owner = jax.vmap(lambda own, number: routed_block(jax.random.fold_in(streams_of[2], 2), own, number, 4 * E_DEV, N_GRP, 1, CAP, 2))(phys_owner_keys, phys_owner_turns).reshape((ELEMS, 4, 1))
    neighbours = draw_neighbours(jax.random.fold_in(streams_of[7], 71), 0)
    phys_rate = jnp.clip(jnp.exp(math.log(2.0) - 2.3025851 * jax.random.uniform(streams_of[4], (NLEV, SLOTS), jnp.float32) ** shard_levels(streams_of[4], (NLEV, SLOTS), ((1, 768),), -0.2, 0.2)), 0.2, 2.0)
    phys_forcing = centred(streams_of[5], (NLEV, SLOTS), 1.0, 6.0, ((1, 768),), jnp.float32)
    field_mix = centred(streams_of[6], (NF, NF), NF ** -0.5, 2.0, (), jnp.float32)
    return dict(gll_state=gll_state, metric=metric, phys_owner=phys_owner, neighbours=neighbours, phys_rate=phys_rate, phys_forcing=phys_forcing, field_mix=field_mix)


def lagrange_value(gll_nodes, node_index, point):
    value = 1.0
    for other_index in range(4):
        if other_index != node_index:
            value = value * (point - gll_nodes[other_index]) / (gll_nodes[node_index] - gll_nodes[other_index])
    return value

def remap_tables():
    gll_nodes = np.array([-1.0, -1.0 / np.sqrt(5.0), 1.0 / np.sqrt(5.0), 1.0])
    offset = 0.5 / np.sqrt(3.0)
    halves = np.zeros((2, 4))
    for node_index in range(4):
        left_sum = lagrange_value(gll_nodes, node_index, -0.5 - offset) + lagrange_value(gll_nodes, node_index, -0.5 + offset)
        right_sum = lagrange_value(gll_nodes, node_index, 0.5 - offset) + lagrange_value(gll_nodes, node_index, 0.5 + offset)
        halves[0, node_index] = 0.5 * left_sum
        halves[1, node_index] = 0.5 * right_sum
    cell_weights = (halves[None, :, None, :] * halves[:, None, :, None]).reshape(4, 16)
    interp_cols = np.stack([0.5 - gll_nodes, 0.5 + gll_nodes], axis=1)
    cell_to_node = (interp_cols[None, :, None, :] * interp_cols[:, None, :, None]).reshape(16, 4)
    node_x = np.tile(gll_nodes, 4)
    node_y = np.repeat(gll_nodes, 4)
    slope_weights = 0.5 * np.stack([np.maximum(0.0, -node_x), np.maximum(0.0, node_x), np.maximum(0.0, -node_y), np.maximum(0.0, node_y)], axis=1)
    return (jnp.asarray(cell_weights, jnp.float32), jnp.asarray(cell_to_node, jnp.float32), jnp.asarray(slope_weights, jnp.float32))

def to_cells(gll_state, metric):
    cell_weights, cell_to_node, slope_weights = remap_tables()
    weighted = cell_weights[:, :, None] * metric[None, :, :]
    cell_area = lax.optimization_barrier(jnp.sum(weighted, axis=1))
    cell_mass = jnp.einsum('cne,flne->flce', weighted, gll_state, precision=lax.Precision.HIGHEST)
    return cell_mass / cell_area[None, None]

def physics(cell_values, relax_rate, forcing, field_mix):
    mixed_fields = jnp.einsum('fg,g...->f...', field_mix, cell_values, precision=lax.Precision.HIGHEST)
    return relax_rate[None] * jnp.tanh(mixed_fields + forcing[None])

def to_nodes(tendency, neighbour_means):
    cell_weights, cell_to_node, slope_weights = remap_tables()
    own_mean = lax.optimization_barrier(jnp.mean(tendency, axis=2))
    reconstructed = jnp.einsum('nc,flce->flne', cell_to_node, tendency, precision=lax.Precision.HIGHEST)
    reconstructed = reconstructed + jnp.einsum('nk,flke->flne', slope_weights, neighbour_means - own_mean[:, :, None], precision=lax.Precision.HIGHEST)
    lower_bound = jnp.minimum(lax.optimization_barrier(jnp.min(tendency, axis=2)), lax.optimization_barrier(jnp.min(neighbour_means, axis=2)))
    upper_bound = jnp.maximum(lax.optimization_barrier(jnp.max(tendency, axis=2)), lax.optimization_barrier(jnp.max(neighbour_means, axis=2)))
    return jnp.clip(reconstructed, lower_bound[:, :, None], upper_bound[:, :, None])

def reference(gll_state, metric, phys_owner, neighbours, phys_rate, phys_forcing, field_mix):
    device_total = N_GRP * N_ROW
    cell_values = to_cells(gll_state, metric)
    owner_grp = phys_owner[:, :, 0].reshape(device_total, 4 * E_DEV)
    onehot = (owner_grp[:, :, None] == jnp.arange(N_GRP, dtype=jnp.int32)[None, None, :]).astype(jnp.int32)
    slot_rank = lax.optimization_barrier(jnp.sum((jnp.cumsum(onehot, axis=1) - onehot) * onehot, axis=2))
    device_index = jnp.arange(device_total, dtype=jnp.int32)[:, None]
    target = ((owner_grp * N_ROW + device_index % N_ROW) * (N_GRP * CAP) + device_index // N_ROW * CAP + slot_rank).astype(jnp.int32)
    target = target.reshape(device_total * E_DEV, 4).T
    relax_rate = phys_rate[:, target]
    forcing = phys_forcing[:, target]
    tendency = physics(cell_values, relax_rate, forcing, field_mix)
    own_mean = lax.optimization_barrier(jnp.mean(tendency, axis=2))
    neighbour_means = own_mean[:, :, neighbours]
    return to_nodes(tendency, neighbour_means)
```

```python
import functools

import jax
import jax.numpy as jnp
import numpy as np
from jax import lax
from jax.experimental import pallas as pl
from jax.experimental.pallas import tpu as pltpu
from jax.sharding import PartitionSpec as P

MESH = pl.DeviceIdType.MESH
F32 = jnp.float32
BF16 = jnp.bfloat16
HIGH = 11


def lagrange_value(gll_nodes, node_index, point):
    value = 1.0
    for other_index in range(4):
        if other_index != node_index:
            value = (
                value
                * (point - gll_nodes[other_index])
                / (gll_nodes[node_index] - gll_nodes[other_index])
            )
    return value


def cell_weights():
    gll_nodes = np.array([-1.0, -1.0 / np.sqrt(5.0), 1.0 / np.sqrt(5.0), 1.0])
    offset = 0.5 / np.sqrt(3.0)
    halves = np.zeros((2, 4))
    for i in range(4):
        halves[0, i] = 0.5 * (
            lagrange_value(gll_nodes, i, -0.5 - offset)
            + lagrange_value(gll_nodes, i, -0.5 + offset)
        )
        halves[1, i] = 0.5 * (
            lagrange_value(gll_nodes, i, 0.5 - offset) + lagrange_value(gll_nodes, i, 0.5 + offset)
        )
    return (halves[None, :, None, :] * halves[:, None, :, None]).reshape(4, 16)


def exchange_kernel(
    n_grp,
    n_row,
    n_x,
    gll_hbm,
    metric_hbm,
    owner_hbm,
    rate_hbm,
    forcing_hbm,
    mix_hbm,
    tend_ref,
    low_ref,
    high_ref,
    gbuf,
    metric_ref,
    owner_ref,
    rate_ref,
    forcing_ref,
    mix_ref,
    wbuf,
    slots_t,
    send,
    recv,
    rows,
    onehot,
    cells,
    edge_out,
    edge_in,
    in_sem,
    gll_sem,
    send_sem,
    recv_sem,
    edge_send_sem,
    edge_recv_sem,
):
    fields = gll_hbm.shape[0]
    n_z = n_grp // n_x
    me = lax.axis_index("grp")
    my_row = lax.axis_index("row")
    my_z, my_x = me // n_x, me % n_x

    small = [
        pltpu.make_async_copy(src, dst, in_sem.at[k])
        for k, (src, dst) in enumerate(
            (
                (rate_hbm, rate_ref),
                (forcing_hbm, forcing_ref),
                (metric_hbm, metric_ref),
                (owner_hbm, owner_ref),
                (mix_hbm, mix_ref),
            )
        )
    ]
    for copy in small:
        copy.start()
    gll_copies = [
        pltpu.make_async_copy(gll_hbm.at[f], gbuf.at[f], gll_sem.at[f]) for f in range(fields)
    ]
    for copy in gll_copies:
        copy.start()

    here = me * n_row + my_row
    total = n_grp * n_row
    after = lax.rem(here + 1, total)
    before = lax.rem(here + total - 1, total)
    sides = [(d // n_row, d % n_row) for d in (before, after)]

    def partner(i):
        m = i // n_x
        half = (m + 1) // 2
        dz = n_z // 2 + half * (1 - 2 * (m % 2))
        dx = n_x - 1 - i % n_x
        there = ((my_z + dz) % n_z) * n_x + (my_x + dx) % n_x
        origin = ((my_z - dz + n_z) % n_z) * n_x + (my_x - dx + n_x) % n_x
        return there, origin

    barrier = pltpu.get_barrier_semaphore()

    def greet(i, carry):
        there, _ = partner(i)
        pl.semaphore_signal(barrier, inc=1, device_id=(there, my_row), device_id_type=MESH)
        return carry

    for side in sides:
        pl.semaphore_signal(barrier, inc=1, device_id=side, device_id_type=MESH)
    lax.fori_loop(0, n_grp - 1, greet, 0)

    small[0].wait()
    small[1].wait()
    slot_count = rate_ref.shape[1]
    for k in range(0, slot_count, 128):
        width = min(128, slot_count - k)
        r = rate_ref[:, k : k + width]
        f = forcing_ref[:, k : k + width]
        slots_t[k : k + width, :] = jnp.concatenate([r, f, r, f], axis=0).T
    lane = lax.broadcasted_iota(jnp.int32, (HIGH, 128), 1)
    for g in range(n_grp):
        at = 2 * HIGH * g
        send[g] = jnp.where(lane < 64, slots_t[at : at + HIGH], slots_t[at + HIGH : at + 2 * HIGH])

    small[2].wait()
    table = cell_weights()
    for c in range(4):
        weighted = [metric_ref[n : n + 1, :] * float(table[c, n]) for n in range(16)]
        area = functools.reduce(lambda a, b: a + b, weighted)
        inverse = 1.0 / area
        for n in range(16):
            wbuf[16 * c + n : 16 * c + n + 1, :] = weighted[n] * inverse

    levels = tend_ref.shape[2]
    for copy in gll_copies:
        copy.wait()

    def to_cells(f, carry):
        sums = [None] * 4
        for n in range(16):
            g = gbuf[f, pl.ds(n, levels, stride=16), :]
            for c in range(4):
                term = wbuf[16 * c + n : 16 * c + n + 1, :] * g
                sums[c] = term if sums[c] is None else sums[c] + term
        for c in range(4):
            cells[f, c] = sums[c]
        return carry

    lax.fori_loop(0, fields, to_cells, 0)

    pl.semaphore_wait(barrier, n_grp + 1)

    def block_copy(i):
        there, _ = partner(i)
        return pltpu.make_async_remote_copy(
            src_ref=send.at[there],
            dst_ref=recv.at[me],
            send_sem=send_sem.at[i],
            recv_sem=recv_sem.at[i],
            device_id=(there, my_row),
            device_id_type=MESH,
        )

    def start_block(i, carry):
        block_copy(i).start()
        return carry

    lax.fori_loop(0, n_grp - 1, start_block, 0)

    small[4].wait()

    def mix(i, carry):
        c, at = i // (levels // 8), pl.multiple_of((i % (levels // 8)) * 8, 8)
        block = [cells[g, c, pl.ds(at, 8), :] for g in range(fields)]
        for f in range(fields):
            total_f = mix_ref[f, 0] * block[0]
            for g in range(1, fields):
                total_f = total_f + mix_ref[f, g] * block[g]
            cells[f, c, pl.ds(at, 8), :] = total_f
        return carry

    lax.fori_loop(0, 4 * (levels // 8), mix, 0)

    small[3].wait()
    grp_ids = lax.broadcasted_iota(jnp.int32, (n_grp, 128), 0)
    owners = [owner_ref[c : c + 1, :] for c in range(4)]
    match = [jnp.where(grp_ids == owners[c], 1.0, 0.0).astype(F32) for c in range(4)]
    count = match[0] + match[1] + match[2] + match[3]
    before_e = lax.broadcasted_iota(jnp.int32, (128, 128), 0) < lax.broadcasted_iota(
        jnp.int32, (128, 128), 1
    )
    running = jnp.dot(
        count.astype(BF16),
        jnp.where(before_e, 1.0, 0.0).astype(BF16),
        preferred_element_type=F32,
    )
    upper = []
    row_ids = lax.broadcasted_iota(jnp.int32, (256, 128), 0)
    for c in range(4):
        rank = jnp.sum(match[c] * running, axis=0, keepdims=True).astype(jnp.int32)
        running = running + match[c]
        is_upper = rank >= HIGH
        upper.append(is_upper)
        key = owners[c] * 16 + jnp.where(is_upper, rank - HIGH, rank)
        for k in range(n_grp * 16 // 256):
            onehot[256 * k : 256 * k + 256, 128 * c : 128 * c + 128] = jnp.where(
                row_ids == key - 256 * k, 1.0, 0.0
            ).astype(BF16)

    rows[...] = jnp.zeros_like(rows)
    recv[me] = send[me]

    def land(i, carry):
        block_copy(i).wait_recv()
        return carry

    lax.fori_loop(0, n_grp - 1, land, 0)
    for g in range(n_grp):
        rows[16 * g : 16 * g + HIGH, :] = recv[g]

    picked = None
    for k in range(n_grp * 16 // 256):
        block = rows[256 * k : 256 * k + 256, :].T
        top = block.astype(BF16)
        rest = (block - top.astype(F32)).astype(BF16)
        hot = onehot[256 * k : 256 * k + 256, :]
        part = jnp.dot(top, hot, preferred_element_type=F32) + jnp.dot(
            rest, hot, preferred_element_type=F32
        )
        picked = part if picked is None else picked + part

    for c in range(4):
        cut = picked[:, 128 * c : 128 * c + 128]
        both = jnp.where(upper[c], cut[64:128], cut[0:64])
        for f in range(fields):
            tend_ref[f, c] = both[:levels] * jnp.tanh(cells[f, c] + both[levels:])

    lanes = lax.broadcasted_iota(jnp.int32, (levels, 128), 1)
    for half in range(2):
        first, last = None, None
        for q in range(fields // 2):
            f = 2 * q + half
            mean = 0.25 * ((tend_ref[f, 0] + tend_ref[f, 1]) + (tend_ref[f, 2] + tend_ref[f, 3]))
            inside = (lanes >= 32 * q) & (lanes < 32 * q + 32)
            low = pltpu.roll(mean, 32 * q, 1) if q else mean
            high = pltpu.roll(mean, (32 * q + 32) % 128, 1) if (32 * q + 32) % 128 else mean
            first = low if first is None else jnp.where(inside, low, first)
            last = high if last is None else jnp.where(inside, high, last)
        edge_out[0, half * levels : half * levels + levels, :] = first
        edge_out[1, half * levels : half * levels + levels, :] = last

    edge_copies = [
        pltpu.make_async_remote_copy(
            src_ref=edge_out.at[k],
            dst_ref=edge_in.at[1 - k],
            send_sem=edge_send_sem.at[k],
            recv_sem=edge_recv_sem.at[k],
            device_id=sides[k],
            device_id_type=MESH,
        )
        for k in range(2)
    ]
    for copy in edge_copies:
        copy.start()

    def sent(i, carry):
        block_copy(i).wait_send()
        return carry

    lax.fori_loop(0, n_grp - 1, sent, 0)
    for copy in edge_copies:
        copy.wait()
    low_ref[...] = edge_in[0]
    high_ref[...] = edge_in[1]


def nodes_kernel(elems_total, n_row, tend_ref, low_ref, high_ref, near_ref, out_ref, scratch):
    q = pl.program_id(0)
    levels, width = tend_ref.shape[2], tend_ref.shape[3]
    here = (lax.axis_index("grp") * n_row + lax.axis_index("row")) * width
    elem = lax.broadcasted_iota(jnp.int32, (4, width), 1)
    away = near_ref[...] - (here + elem)
    away = jnp.where(away > elems_total // 2, away - elems_total, away)
    away = jnp.where(away < -(elems_total // 2), away + elems_total, away)
    place = elem + away
    inner = jnp.clip(place, 0, width - 1)
    outer = jnp.where(place < 0, place + 32, place - width) + 32 * q
    outer = jnp.clip(outer, 0, width - 1)
    inside = (place >= 0) & (place < width)

    def pick(values, index):
        return jnp.take_along_axis(values, index, axis=1, mode="promise_in_bounds")

    sub = lax.broadcasted_iota(jnp.int32, (8, width), 0)
    g1 = float(1.0 / np.sqrt(5.0))
    i_of = sub % 4
    g_i = jnp.where(i_of == 0, -1.0, jnp.where(i_of == 1, -g1, jnp.where(i_of == 2, g1, 1.0)))
    west_side = i_of < 2
    g_south = jnp.where(sub < 4, -1.0, -g1)
    g_north = jnp.where(sub < 4, g1, 1.0)

    for h in range(2):
        for b in range(levels // 8):
            at = slice(8 * b, 8 * b + 8)
            t = [tend_ref[h, c, at, :] for c in range(4)]
            mean = 0.25 * ((t[0] + t[1]) + (t[2] + t[3]))
            near = []
            halo_at = slice(h * levels + 8 * b, h * levels + 8 * b + 8)
            for k in range(4):
                halo = (low_ref if k % 2 == 0 else high_ref)[halo_at, :]
                own_pick = pick(mean, jnp.broadcast_to(inner[k : k + 1], (8, width)))
                halo_pick = pick(halo, jnp.broadcast_to(outer[k : k + 1], (8, width)))
                near.append(
                    jnp.where(jnp.broadcast_to(inside[k : k + 1], (8, width)), own_pick, halo_pick)
                )
            low = functools.reduce(jnp.minimum, t + near)
            high = functools.reduce(jnp.maximum, t + near)
            slope_x = 0.5 * ((t[1] + t[3]) - (t[0] + t[2]))
            slope_y = 0.5 * ((t[2] + t[3]) - (t[0] + t[1]))
            cross = (t[3] - t[2]) - (t[1] - t[0])
            scratch[0, at, :] = mean
            scratch[1, at, :] = slope_x - 0.5 * (near[0] - mean)
            scratch[2, at, :] = slope_x + 0.5 * (near[1] - mean)
            scratch[3, at, :] = slope_y - 0.5 * (near[2] - mean)
            scratch[4, at, :] = slope_y + 0.5 * (near[3] - mean)
            scratch[5, at, :] = cross
            scratch[6, at, :] = low
            scratch[7, at, :] = high
        for l in range(levels):
            mean, x_west, x_east, y_south, y_north, cross, low, high = (
                jnp.broadcast_to(scratch[k, l : l + 1, :], (8, width)) for k in range(8)
            )
            base = mean + g_i * jnp.where(west_side, x_west, x_east)
            twist = g_i * cross
            out_ref[h, l, 0:8, :] = jnp.minimum(
                jnp.maximum(base + g_south * (y_south + twist), low), high
            )
            out_ref[h, l, 8:16, :] = jnp.minimum(
                jnp.maximum(base + g_north * (y_north + twist), low), high
            )


def on_device(n_grp, n_row, n_x, gll_state, metric, phys_owner, neighbours, rate, forcing, mix):
    fields, levels, nodes, elems = gll_state.shape
    slots = rate.shape[1]
    hbm = pl.BlockSpec(memory_space=pl.ANY)
    vmem = pl.BlockSpec(memory_space=pltpu.VMEM)
    tend, low, high = pl.pallas_call(
        functools.partial(exchange_kernel, n_grp, n_row, n_x),
        out_shape=(
            jax.ShapeDtypeStruct((fields, 4, levels, elems), F32),
            jax.ShapeDtypeStruct((2 * levels, elems), F32),
            jax.ShapeDtypeStruct((2 * levels, elems), F32),
        ),
        in_specs=[hbm] * 6,
        out_specs=(vmem, vmem, vmem),
        scratch_shapes=[
            pltpu.VMEM((fields, levels * nodes, elems), F32),
            pltpu.VMEM((nodes, elems), F32),
            pltpu.VMEM((4, elems), jnp.int32),
            pltpu.VMEM((levels, slots), F32),
            pltpu.VMEM((levels, slots), F32),
            pltpu.SMEM((fields, fields), F32),
            pltpu.VMEM((64, elems), F32),
            pltpu.VMEM((slots, 128), F32),
            pltpu.VMEM((n_grp, HIGH, 128), F32),
            pltpu.VMEM((n_grp, HIGH, 128), F32),
            pltpu.VMEM((n_grp * 16, 128), F32),
            pltpu.VMEM((n_grp * 16, 4 * elems), BF16),
            pltpu.VMEM((fields, 4, levels, elems), F32),
            pltpu.VMEM((2, 2 * levels, elems), F32),
            pltpu.VMEM((2, 2 * levels, elems), F32),
            pltpu.SemaphoreType.DMA((5,)),
            pltpu.SemaphoreType.DMA((fields,)),
            pltpu.SemaphoreType.DMA((n_grp - 1,)),
            pltpu.SemaphoreType.DMA((n_grp - 1,)),
            pltpu.SemaphoreType.DMA((2,)),
            pltpu.SemaphoreType.DMA((2,)),
        ],
        compiler_params=pltpu.CompilerParams(collective_id=0, has_side_effects=True),
        name="exchange",
    )(
        gll_state.reshape(fields, levels * nodes, elems),
        metric,
        phys_owner[:, :, 0].T,
        rate,
        forcing,
        mix,
    )
    return pl.pallas_call(
        functools.partial(nodes_kernel, elems * n_grp * n_row, n_row),
        grid=(fields // 2,),
        out_shape=jax.ShapeDtypeStruct(gll_state.shape, F32),
        in_specs=[
            pl.BlockSpec((2, 4, levels, elems), lambda i: (i, 0, 0, 0)),
            pl.BlockSpec((2 * levels, elems), lambda i: (0, 0)),
            pl.BlockSpec((2 * levels, elems), lambda i: (0, 0)),
            pl.BlockSpec((4, elems), lambda i: (0, 0)),
        ],
        out_specs=pl.BlockSpec((2, levels, nodes, elems), lambda i: (i, 0, 0, 0)),
        scratch_shapes=[pltpu.VMEM((8, levels, elems), F32)],
        name="nodes",
    )(tend, low, high, neighbours)


def solution(mesh):
    in_specs = (
        P(None, None, None, ("grp", "row")),
        P(None, ("grp", "row")),
        P(("grp", "row"), None, None),
        P(None, ("grp", "row")),
        P(None, ("grp", "row")),
        P(None, ("grp", "row")),
        P(),
    )
    out_specs = P(None, None, None, ("grp", "row"))
    n_grp, n_row = mesh.shape["grp"], mesh.shape["row"]
    return jax.shard_map(
        functools.partial(on_device, n_grp, n_row, 4),
        mesh=mesh,
        in_specs=in_specs,
        out_specs=out_specs,
        check_vma=False,
    )
```

```python
import functools

import jax
import jax.numpy as jnp
import numpy as np
from jax import lax
from jax.experimental import pallas as pl
from jax.experimental.pallas import tpu as pltpu
from jax.sharding import PartitionSpec as P

MESH = pl.DeviceIdType.MESH
F32 = jnp.float32
BF16 = jnp.bfloat16
HIGH = 11


def lagrange_value(gll_nodes, node_index, point):
    value = 1.0
    for other_index in range(4):
        if other_index != node_index:
            value = (
                value
                * (point - gll_nodes[other_index])
                / (gll_nodes[node_index] - gll_nodes[other_index])
            )
    return value


def cell_weights():
    gll_nodes = np.array([-1.0, -1.0 / np.sqrt(5.0), 1.0 / np.sqrt(5.0), 1.0])
    offset = 0.5 / np.sqrt(3.0)
    halves = np.zeros((2, 4))
    for i in range(4):
        halves[0, i] = 0.5 * (
            lagrange_value(gll_nodes, i, -0.5 - offset)
            + lagrange_value(gll_nodes, i, -0.5 + offset)
        )
        halves[1, i] = 0.5 * (
            lagrange_value(gll_nodes, i, 0.5 - offset) + lagrange_value(gll_nodes, i, 0.5 + offset)
        )
    return (halves[None, :, None, :] * halves[:, None, :, None]).reshape(4, 16)


def exchange_kernel(
    n_grp,
    n_row,
    gll_hbm,
    metric_hbm,
    owner_hbm,
    rate_hbm,
    forcing_hbm,
    mix_hbm,
    tend_ref,
    low_ref,
    high_ref,
    gbuf,
    metric_ref,
    owner_ref,
    rate_ref,
    forcing_ref,
    mix_ref,
    wbuf,
    slots_t,
    send,
    recv,
    rows,
    onehot,
    cells,
    edge_out,
    edge_in,
    in_sem,
    gll_sem,
    send_sem,
    recv_sem,
    edge_send_sem,
    edge_recv_sem,
    ready,
    edge_ready,
):
    fields = gll_hbm.shape[0]
    me = lax.axis_index("grp")
    my_row = lax.axis_index("row")

    small = [
        pltpu.make_async_copy(src, dst, in_sem.at[k])
        for k, (src, dst) in enumerate(
            (
                (rate_hbm, rate_ref),
                (forcing_hbm, forcing_ref),
                (metric_hbm, metric_ref),
                (owner_hbm, owner_ref),
                (mix_hbm, mix_ref),
            )
        )
    ]
    for copy in small:
        copy.start()
    gll_copies = [
        pltpu.make_async_copy(gll_hbm.at[f], gbuf.at[f], gll_sem.at[f]) for f in range(fields)
    ]
    for copy in gll_copies:
        copy.start()

    here = me * n_row + my_row
    total = n_grp * n_row
    after = lax.rem(here + 1, total)
    before = lax.rem(here + total - 1, total)
    sides = [(d // n_row, d % n_row) for d in (before, after)]

    barrier = pltpu.get_barrier_semaphore()

    def greet(g, carry):
        pl.semaphore_signal(barrier, inc=1, device_id=(g, my_row), device_id_type=MESH)
        return carry

    lax.fori_loop(me + 1, n_grp, greet, 0)

    @pl.when(here < total - 1)
    def _():
        pl.semaphore_signal(barrier, inc=1, device_id=sides[1], device_id_type=MESH)

    @pl.when(here == 0)
    def _():
        pl.semaphore_signal(barrier, inc=1, device_id=sides[0], device_id_type=MESH)

    small[0].wait()
    small[1].wait()
    slot_count = rate_ref.shape[1]
    for k in range(0, slot_count, 128):
        width = min(128, slot_count - k)
        r = rate_ref[:, k : k + width]
        f = forcing_ref[:, k : k + width]
        slots_t[k : k + width, :] = jnp.concatenate([r, f, r, f], axis=0).T
    lane = lax.broadcasted_iota(jnp.int32, (HIGH, 128), 1)
    for g in range(n_grp):
        at = 2 * HIGH * g
        send[g] = jnp.where(lane < 64, slots_t[at : at + HIGH], slots_t[at + HIGH : at + 2 * HIGH])

    below = jnp.where(here > 0, 1, 0) + jnp.where(here == total - 1, 1, 0)

    @pl.when(here > 0)
    def _():
        pl.semaphore_wait(barrier, me + below)

    def block_copy(there, origin):
        return pltpu.make_async_remote_copy(
            src_ref=send.at[there],
            dst_ref=recv.at[me],
            send_sem=send_sem.at[there],
            recv_sem=recv_sem.at[origin],
            device_id=(there, my_row),
            device_id_type=MESH,
        )

    def send_down(g, carry):
        block_copy(g, me).start()
        return carry

    lax.fori_loop(0, me, send_down, 0)

    def tell(g, carry):
        pl.semaphore_signal(ready.at[me], inc=1, device_id=(g, my_row), device_id_type=MESH)
        return carry

    lax.fori_loop(0, me, tell, 0)

    @pl.when(here > 0)
    def _():
        pl.semaphore_signal(edge_ready.at[1], inc=1, device_id=sides[0], device_id_type=MESH)

    @pl.when(here == total - 1)
    def _():
        pl.semaphore_signal(edge_ready.at[0], inc=1, device_id=sides[1], device_id_type=MESH)

    small[2].wait()
    table = cell_weights()
    for c in range(4):
        weighted = [metric_ref[n : n + 1, :] * float(table[c, n]) for n in range(16)]
        area = functools.reduce(lambda a, b: a + b, weighted)
        inverse = 1.0 / area
        for n in range(16):
            wbuf[16 * c + n : 16 * c + n + 1, :] = weighted[n] * inverse

    levels = tend_ref.shape[2]
    for copy in gll_copies:
        copy.wait()

    def to_cells(f, carry):
        sums = [None] * 4
        for n in range(16):
            g = gbuf[f, pl.ds(n, levels, stride=16), :]
            for c in range(4):
                term = wbuf[16 * c + n : 16 * c + n + 1, :] * g
                sums[c] = term if sums[c] is None else sums[c] + term
        for c in range(4):
            cells[f, c] = sums[c]
        return carry

    lax.fori_loop(0, fields, to_cells, 0)

    small[4].wait()

    def mix(i, carry):
        c, at = i // (levels // 8), pl.multiple_of((i % (levels // 8)) * 8, 8)
        block = [cells[g, c, pl.ds(at, 8), :] for g in range(fields)]
        for f in range(fields):
            total_f = mix_ref[f, 0] * block[0]
            for g in range(1, fields):
                total_f = total_f + mix_ref[f, g] * block[g]
            cells[f, c, pl.ds(at, 8), :] = total_f
        return carry

    lax.fori_loop(0, 4 * (levels // 8), mix, 0)

    small[3].wait()
    grp_ids = lax.broadcasted_iota(jnp.int32, (n_grp, 128), 0)
    owners = [owner_ref[c : c + 1, :] for c in range(4)]
    match = [jnp.where(grp_ids == owners[c], 1.0, 0.0).astype(F32) for c in range(4)]
    count = match[0] + match[1] + match[2] + match[3]
    before_e = lax.broadcasted_iota(jnp.int32, (128, 128), 0) < lax.broadcasted_iota(
        jnp.int32, (128, 128), 1
    )
    running = jnp.dot(
        count.astype(BF16),
        jnp.where(before_e, 1.0, 0.0).astype(BF16),
        preferred_element_type=F32,
    )
    upper = []
    row_ids = lax.broadcasted_iota(jnp.int32, (256, 128), 0)
    for c in range(4):
        rank = jnp.sum(match[c] * running, axis=0, keepdims=True).astype(jnp.int32)
        running = running + match[c]
        is_upper = rank >= HIGH
        upper.append(is_upper)
        key = owners[c] * 16 + jnp.where(is_upper, rank - HIGH, rank)
        for k in range(n_grp * 16 // 256):
            onehot[256 * k : 256 * k + 256, 128 * c : 128 * c + 128] = jnp.where(
                row_ids == key - 256 * k, 1.0, 0.0
            ).astype(BF16)

    rows[...] = jnp.zeros_like(rows)
    recv[me] = send[me]

    def send_up(g, carry):
        pl.semaphore_wait(ready.at[g], 1)
        block_copy(g, me).start()
        return carry

    lax.fori_loop(me + 1, n_grp, send_up, 0)

    picked = None
    for k in range(n_grp // 16):
        for g in range(16 * k, 16 * k + 16):

            @pl.when(g != me)
            def _():
                block_copy(me, g).wait_recv()

            rows[16 * g : 16 * g + HIGH, :] = recv[g]
        block = rows[256 * k : 256 * k + 256, :].T
        top = block.astype(BF16)
        rest = (block - top.astype(F32)).astype(BF16)
        hot = onehot[256 * k : 256 * k + 256, :]
        part = jnp.dot(top, hot, preferred_element_type=F32) + jnp.dot(
            rest, hot, preferred_element_type=F32
        )
        picked = part if picked is None else picked + part

    for c in range(4):
        cut = picked[:, 128 * c : 128 * c + 128]
        both = jnp.where(upper[c], cut[64:128], cut[0:64])
        for f in range(fields):
            tend_ref[f, c] = both[:levels] * jnp.tanh(cells[f, c] + both[levels:])

    lanes = lax.broadcasted_iota(jnp.int32, (levels, 128), 1)
    for half in range(2):
        first, last = None, None
        for q in range(fields // 2):
            f = 2 * q + half
            mean = 0.25 * ((tend_ref[f, 0] + tend_ref[f, 1]) + (tend_ref[f, 2] + tend_ref[f, 3]))
            inside = (lanes >= 32 * q) & (lanes < 32 * q + 32)
            low = pltpu.roll(mean, 32 * q, 1) if q else mean
            high = pltpu.roll(mean, (32 * q + 32) % 128, 1) if (32 * q + 32) % 128 else mean
            first = low if first is None else jnp.where(inside, low, first)
            last = high if last is None else jnp.where(inside, high, last)
        edge_out[0, half * levels : half * levels + levels, :] = first
        edge_out[1, half * levels : half * levels + levels, :] = last

    edge_copies = [
        pltpu.make_async_remote_copy(
            src_ref=edge_out.at[k],
            dst_ref=edge_in.at[1 - k],
            send_sem=edge_send_sem.at[k],
            recv_sem=edge_recv_sem.at[k],
            device_id=sides[k],
            device_id_type=MESH,
        )
        for k in range(2)
    ]

    @pl.when(here == 0)
    def _():
        pl.semaphore_wait(edge_ready.at[0], 1)

    @pl.when(here < total - 1)
    def _():
        pl.semaphore_wait(edge_ready.at[1], 1)

    for copy in edge_copies:
        copy.start()

    def sent(g, carry):
        @pl.when(g != me)
        def _():
            block_copy(g, me).wait_send()

        return carry

    lax.fori_loop(0, n_grp, sent, 0)
    for copy in edge_copies:
        copy.wait()
    low_ref[...] = edge_in[0]
    high_ref[...] = edge_in[1]


def nodes_kernel(
    elems_total, n_row, tend_ref, low_ref, high_ref, near_ref, out_hbm, done, scratch, sems
):
    fields, _, levels, width = tend_ref.shape
    here = (lax.axis_index("grp") * n_row + lax.axis_index("row")) * width
    elem = lax.broadcasted_iota(jnp.int32, (4, width), 1)
    away = near_ref[...] - (here + elem)
    away = jnp.where(away > elems_total // 2, away - elems_total, away)
    away = jnp.where(away < -(elems_total // 2), away + elems_total, away)
    place = elem + away
    inner = jnp.clip(place, 0, width - 1)
    outer = jnp.clip(jnp.where(place < 0, place + 32, place - width), 0, 31)
    inside = (place >= 0) & (place < width)

    def all_rows(x, k):
        return jnp.broadcast_to(x[k : k + 1], (8, width))

    inner = [all_rows(inner, k) for k in range(4)]
    outer = [all_rows(outer, k) for k in range(4)]
    inside = [all_rows(inside, k) for k in range(4)]

    def pick(values, index):
        return jnp.take_along_axis(values, index, axis=1, mode="promise_in_bounds")

    sub = lax.broadcasted_iota(jnp.int32, (8, width), 0)
    g1 = float(1.0 / np.sqrt(5.0))
    i_of = sub % 4
    g_i = jnp.where(i_of == 0, -1.0, jnp.where(i_of == 1, -g1, jnp.where(i_of == 2, g1, 1.0)))
    west_side = i_of < 2
    g_south = jnp.where(sub < 4, -1.0, -g1)
    g_north = jnp.where(sub < 4, g1, 1.0)

    def write(f):
        return pltpu.make_async_copy(done.at[f], out_hbm.at[f], sems.at[f])

    def field(f, carry):
        shift = 32 * (f // 2)
        for b in range(levels // 8):
            at = slice(8 * b, 8 * b + 8)
            t = [tend_ref[f, c, at, :] for c in range(4)]
            mean = 0.25 * ((t[0] + t[1]) + (t[2] + t[3]))
            halo_at = pl.ds(pl.multiple_of((f % 2) * levels + 8 * b, 8), 8)
            halos = (low_ref[halo_at, :], high_ref[halo_at, :])
            near = []
            for k in range(4):
                if k < 2:
                    own_pick = pltpu.roll(mean, 1 if k == 0 else width - 1, 1)
                else:
                    own_pick = pick(mean, inner[k])
                halo_pick = pick(halos[k % 2], outer[k] + shift)
                near.append(jnp.where(inside[k], own_pick, halo_pick))
            low = functools.reduce(jnp.minimum, t + near)
            high = functools.reduce(jnp.maximum, t + near)
            slope_x = 0.5 * ((t[1] + t[3]) - (t[0] + t[2]))
            slope_y = 0.5 * ((t[2] + t[3]) - (t[0] + t[1]))
            scratch[0, at, :] = mean
            scratch[1, at, :] = slope_x - 0.5 * (near[0] - mean)
            scratch[2, at, :] = slope_x + 0.5 * (near[1] - mean)
            scratch[3, at, :] = slope_y - 0.5 * (near[2] - mean)
            scratch[4, at, :] = slope_y + 0.5 * (near[3] - mean)
            scratch[5, at, :] = (t[3] - t[2]) - (t[1] - t[0])
            scratch[6, at, :] = low
            scratch[7, at, :] = high
        for l in range(levels):
            mean, x_west, x_east, y_south, y_north, cross, low, high = (
                jnp.broadcast_to(scratch[k, l : l + 1, :], (8, width)) for k in range(8)
            )
            base = mean + g_i * jnp.where(west_side, x_west, x_east)
            twist = g_i * cross
            done[f, l, 0:8, :] = jnp.minimum(
                jnp.maximum(base + g_south * (y_south + twist), low), high
            )
            done[f, l, 8:16, :] = jnp.minimum(
                jnp.maximum(base + g_north * (y_north + twist), low), high
            )
        write(f).start()
        return carry

    lax.fori_loop(0, fields, field, 0)
    for f in range(fields):
        write(f).wait()


def on_device(n_grp, n_row, gll_state, metric, phys_owner, neighbours, rate, forcing, mix):
    fields, levels, nodes, elems = gll_state.shape
    slots = rate.shape[1]
    hbm = pl.BlockSpec(memory_space=pltpu.HBM)
    vmem = pl.BlockSpec(memory_space=pltpu.VMEM)
    tend, low, high = pl.pallas_call(
        functools.partial(exchange_kernel, n_grp, n_row),
        out_shape=(
            jax.ShapeDtypeStruct((fields, 4, levels, elems), F32),
            jax.ShapeDtypeStruct((2 * levels, elems), F32),
            jax.ShapeDtypeStruct((2 * levels, elems), F32),
        ),
        in_specs=[hbm] * 6,
        out_specs=(vmem, vmem, vmem),
        scratch_shapes=[
            pltpu.VMEM((fields, levels * nodes, elems), F32),
            pltpu.VMEM((nodes, elems), F32),
            pltpu.VMEM((4, elems), jnp.int32),
            pltpu.VMEM((levels, slots), F32),
            pltpu.VMEM((levels, slots), F32),
            pltpu.SMEM((fields, fields), F32),
            pltpu.VMEM((64, elems), F32),
            pltpu.VMEM((slots, 128), F32),
            pltpu.VMEM((n_grp, HIGH, 128), F32),
            pltpu.VMEM((n_grp, HIGH, 128), F32),
            pltpu.VMEM((n_grp * 16, 128), F32),
            pltpu.VMEM((n_grp * 16, 4 * elems), BF16),
            pltpu.VMEM((fields, 4, levels, elems), F32),
            pltpu.VMEM((2, 2 * levels, elems), F32),
            pltpu.VMEM((2, 2 * levels, elems), F32),
            pltpu.SemaphoreType.DMA((5,)),
            pltpu.SemaphoreType.DMA((fields,)),
            pltpu.SemaphoreType.DMA((n_grp,)),
            pltpu.SemaphoreType.DMA((n_grp,)),
            pltpu.SemaphoreType.DMA((2,)),
            pltpu.SemaphoreType.DMA((2,)),
            pltpu.SemaphoreType.REGULAR((n_grp,)),
            pltpu.SemaphoreType.REGULAR((2,)),
        ],
        compiler_params=pltpu.CompilerParams(
            collective_id=0, has_side_effects=True, vmem_limit_bytes=16 << 20
        ),
        name="exchange",
    )(
        *(
            pltpu.with_memory_space_constraint(x, pltpu.HBM)
            for x in (
                gll_state.reshape(fields, levels * nodes, elems),
                metric,
                phys_owner[:, :, 0].T,
                rate,
                forcing,
                mix,
            )
        )
    )
    return pl.pallas_call(
        functools.partial(nodes_kernel, elems * n_grp * n_row, n_row),
        out_shape=jax.ShapeDtypeStruct(gll_state.shape, F32),
        in_specs=[vmem] * 4,
        out_specs=hbm,
        scratch_shapes=[
            pltpu.VMEM((fields, levels, nodes, elems), F32),
            pltpu.VMEM((8, levels, elems), F32),
            pltpu.SemaphoreType.DMA((fields,)),
        ],
        compiler_params=pltpu.CompilerParams(vmem_limit_bytes=16 << 20),
        name="nodes",
    )(tend, low, high, neighbours)


def solution(mesh):
    in_specs = (
        P(None, None, None, ("grp", "row")),
        P(None, ("grp", "row")),
        P(("grp", "row"), None, None),
        P(None, ("grp", "row")),
        P(None, ("grp", "row")),
        P(None, ("grp", "row")),
        P(),
    )
    out_specs = P(None, None, None, ("grp", "row"))
    n_grp, n_row = mesh.shape["grp"], mesh.shape["row"]
    return jax.shard_map(
        functools.partial(on_device, n_grp, n_row),
        mesh=mesh,
        in_specs=in_specs,
        out_specs=out_specs,
        check_vma=False,
    )
```

```python
import functools

import jax
import jax.numpy as jnp
import numpy as np
from jax import lax
from jax.experimental import pallas as pl
from jax.experimental.pallas import tpu as pltpu
from jax.sharding import PartitionSpec as P

MESH = pl.DeviceIdType.MESH
F32 = jnp.float32
BF16 = jnp.bfloat16
HIGH = 11


def lagrange_value(gll_nodes, node_index, point):
    value = 1.0
    for other_index in range(4):
        if other_index != node_index:
            value = (
                value
                * (point - gll_nodes[other_index])
                / (gll_nodes[node_index] - gll_nodes[other_index])
            )
    return value


def cell_weights():
    gll_nodes = np.array([-1.0, -1.0 / np.sqrt(5.0), 1.0 / np.sqrt(5.0), 1.0])
    offset = 0.5 / np.sqrt(3.0)
    halves = np.zeros((2, 4))
    for i in range(4):
        halves[0, i] = 0.5 * (
            lagrange_value(gll_nodes, i, -0.5 - offset)
            + lagrange_value(gll_nodes, i, -0.5 + offset)
        )
        halves[1, i] = 0.5 * (
            lagrange_value(gll_nodes, i, 0.5 - offset) + lagrange_value(gll_nodes, i, 0.5 + offset)
        )
    return (halves[None, :, None, :] * halves[:, None, :, None]).reshape(4, 16)


def exchange_kernel(
    n_grp,
    n_row,
    n_x,
    gll_hbm,
    metric_hbm,
    owner_hbm,
    rate_hbm,
    forcing_hbm,
    mix_hbm,
    tend_ref,
    low_ref,
    high_ref,
    gbuf,
    metric_ref,
    owner_ref,
    rate_ref,
    forcing_ref,
    mix_ref,
    wbuf,
    slots_t,
    send,
    recv,
    rows,
    onehot,
    cells,
    edge_out,
    edge_in,
    in_sem,
    sent,
    came,
    edge_send_sem,
    edge_recv_sem,
    ready,
    edge_ready,
):
    fields = gll_hbm.shape[0]
    me = lax.axis_index("grp")
    my_row = lax.axis_index("row")
    n_z = n_grp // n_x
    my_z, my_x = me // n_x, me % n_x

    small = [
        pltpu.make_async_copy(src, dst, in_sem.at[k])
        for k, (src, dst) in enumerate(
            (
                (rate_hbm, rate_ref),
                (forcing_hbm, forcing_ref),
                (metric_hbm, metric_ref),
                (owner_hbm, owner_ref),
                (mix_hbm, mix_ref),
            )
        )
    ]
    for copy in small:
        copy.start()
    gll_copy = pltpu.make_async_copy(gll_hbm, gbuf, in_sem.at[5])
    here = me * n_row + my_row
    total = n_grp * n_row
    after = lax.rem(here + 1, total)
    before = lax.rem(here + total - 1, total)
    sides = [(d // n_row, d % n_row) for d in (before, after)]

    barrier = pltpu.get_barrier_semaphore()

    def greet(g, carry):
        pl.semaphore_signal(barrier, inc=1, device_id=(g, my_row), device_id_type=MESH)
        return carry

    lax.fori_loop(me + 1, n_grp, greet, 0)

    @pl.when(my_row < n_row - 1)
    def _():
        pl.semaphore_signal(barrier, inc=1, device_id=sides[1], device_id_type=MESH)

    @pl.when(my_row == 0)
    def _():
        pl.semaphore_signal(barrier, inc=1, device_id=sides[0], device_id_type=MESH)

    beside = jnp.where(my_row > 0, 1, 0) + jnp.where(my_row == n_row - 1, 1, 0)

    small[0].wait()
    small[1].wait()
    gll_copy.start()
    slot_count = rate_ref.shape[1]
    for k in range(0, slot_count, 128):
        width = min(128, slot_count - k)
        r = rate_ref[:, k : k + width]
        f = forcing_ref[:, k : k + width]
        slots_t[k : k + width, :] = jnp.concatenate([r, f, r, f], axis=0).T
    lane = lax.broadcasted_iota(jnp.int32, (HIGH, 128), 1)
    for g in range(n_grp):
        at = 2 * HIGH * g
        send[g] = jnp.where(lane < 64, slots_t[at : at + HIGH], slots_t[at + HIGH : at + 2 * HIGH])

    @pl.when(here > 0)
    def _():
        pl.semaphore_wait(barrier, me + beside)

    @pl.when(my_row > 0)
    def _():
        pl.semaphore_signal(edge_ready.at[1], inc=1, device_id=sides[0], device_id_type=MESH)

    @pl.when(my_row == n_row - 1)
    def _():
        pl.semaphore_signal(edge_ready.at[0], inc=1, device_id=sides[1], device_id_type=MESH)

    def block_copy(there, origin):
        return pltpu.make_async_remote_copy(
            src_ref=send.at[there],
            dst_ref=recv.at[me],
            send_sem=sent,
            recv_sem=came.at[origin],
            device_id=(there, my_row),
            device_id_type=MESH,
        )

    def tell(g):
        pl.semaphore_signal(ready.at[my_z], inc=1, device_id=(g, my_row), device_id_type=MESH)

    def send_down(z, carry):
        for x in range(n_x):
            tell(z * n_x + x)
            block_copy(z * n_x + x, my_z).start()
        return carry

    lax.fori_loop(0, my_z, send_down, 0)

    def send_beside(g, carry):
        tell(g)
        block_copy(g, my_z).start()
        return carry

    lax.fori_loop(my_z * n_x, me, send_beside, 0)

    small[2].wait()
    table = cell_weights()
    for c in range(4):
        weighted = [metric_ref[n : n + 1, :] * float(table[c, n]) for n in range(16)]
        area = functools.reduce(lambda a, b: a + b, weighted)
        inverse = 1.0 / area
        for n in range(16):
            wbuf[16 * c + n : 16 * c + n + 1, :] = weighted[n] * inverse

    levels = tend_ref.shape[2]
    gll_copy.wait()

    def to_cells(f, carry):
        sums = [None] * 4
        for n in range(16):
            g = gbuf[f, pl.ds(n, levels, stride=16), :]
            for c in range(4):
                term = wbuf[16 * c + n : 16 * c + n + 1, :] * g
                sums[c] = term if sums[c] is None else sums[c] + term
        for c in range(4):
            cells[f, c] = sums[c]
        return carry

    lax.fori_loop(0, fields // 2, to_cells, 0)
    lax.fori_loop(fields // 2, fields, to_cells, 0)

    small[4].wait()

    def mix(i, carry):
        c, at = i // (levels // 8), pl.multiple_of((i % (levels // 8)) * 8, 8)
        block = [cells[g, c, pl.ds(at, 8), :] for g in range(fields)]
        for f in range(fields):
            total_f = mix_ref[f, 0] * block[0]
            for g in range(1, fields):
                total_f = total_f + mix_ref[f, g] * block[g]
            cells[f, c, pl.ds(at, 8), :] = total_f
        return carry

    lax.fori_loop(0, 4 * (levels // 8), mix, 0)

    small[3].wait()
    grp_ids = lax.broadcasted_iota(jnp.int32, (n_grp, 128), 0)
    owners = [owner_ref[c : c + 1, :] for c in range(4)]
    match = [jnp.where(grp_ids == owners[c], 1.0, 0.0).astype(F32) for c in range(4)]
    count = match[0] + match[1] + match[2] + match[3]
    before_e = lax.broadcasted_iota(jnp.int32, (128, 128), 0) < lax.broadcasted_iota(
        jnp.int32, (128, 128), 1
    )
    running = jnp.dot(
        count.astype(BF16),
        jnp.where(before_e, 1.0, 0.0).astype(BF16),
        preferred_element_type=F32,
    )
    upper = []
    row_ids = lax.broadcasted_iota(jnp.int32, (256, 128), 0)
    for c in range(4):
        rank = jnp.sum(match[c] * running, axis=0, keepdims=True).astype(jnp.int32)
        running = running + match[c]
        is_upper = rank >= HIGH
        upper.append(is_upper)
        key = owners[c] * 16 + jnp.where(is_upper, rank - HIGH, rank)
        for k in range(n_grp * 16 // 256):
            onehot[256 * k : 256 * k + 256, 128 * c : 128 * c + 128] = jnp.where(
                row_ids == key - 256 * k, 1.0, 0.0
            ).astype(BF16)

    rows[...] = jnp.zeros_like(rows)
    recv[me] = send[me]

    @pl.when(my_x < n_x - 1)
    def _():
        pl.semaphore_wait(ready.at[my_z], n_x - 1 - my_x)

    def start_up(g, carry):
        block_copy(g, my_z).start()
        return carry

    lax.fori_loop(me + 1, (my_z + 1) * n_x, start_up, 0)

    def send_up(z, carry):
        pl.semaphore_wait(ready.at[z], n_x)
        for x in range(n_x):
            block_copy(z * n_x + x, my_z).start()
        return carry

    lax.fori_loop(my_z + 1, n_z, send_up, 0)

    def bytes_of(what, sem):
        return pltpu.make_async_remote_copy(
            src_ref=what,
            dst_ref=what,
            send_sem=sem,
            recv_sem=sem,
            device_id=sides[0],
            device_id_type=MESH,
        )

    picked = None
    for k in range(n_z // 4):
        for z in range(4 * k, 4 * k + 4):

            @pl.when(z != my_z)
            def _():
                bytes_of(recv.at[pl.ds(0, n_x)], came.at[z]).wait_recv()

            @pl.when(z == my_z)
            def _():
                bytes_of(recv.at[pl.ds(0, n_x - 1)], came.at[z]).wait_recv()

        for g in range(16 * k, 16 * k + 16):
            rows[16 * g : 16 * g + HIGH, :] = recv[g]
        block = rows[256 * k : 256 * k + 256, :].T
        top = block.astype(BF16)
        rest = (block - top.astype(F32)).astype(BF16)
        hot = onehot[256 * k : 256 * k + 256, :]
        part = jnp.dot(top, hot, preferred_element_type=F32) + jnp.dot(
            rest, hot, preferred_element_type=F32
        )
        picked = part if picked is None else picked + part

    for c in range(4):
        cut = picked[:, 128 * c : 128 * c + 128]
        both = jnp.where(upper[c], cut[64:128], cut[0:64])
        for f in range(fields):
            tend_ref[f, c] = both[:levels] * jnp.tanh(cells[f, c] + both[levels:])

    lanes = lax.broadcasted_iota(jnp.int32, (levels, 128), 1)
    for half in range(2):
        first, last = None, None
        for q in range(fields // 2):
            f = 2 * q + half
            mean = 0.25 * ((tend_ref[f, 0] + tend_ref[f, 1]) + (tend_ref[f, 2] + tend_ref[f, 3]))
            inside = (lanes >= 32 * q) & (lanes < 32 * q + 32)
            low = pltpu.roll(mean, 32 * q, 1) if q else mean
            high = pltpu.roll(mean, (32 * q + 32) % 128, 1) if (32 * q + 32) % 128 else mean
            first = low if first is None else jnp.where(inside, low, first)
            last = high if last is None else jnp.where(inside, high, last)
        edge_out[0, half * levels : half * levels + levels, :] = first
        edge_out[1, half * levels : half * levels + levels, :] = last

    edge_copies = [
        pltpu.make_async_remote_copy(
            src_ref=edge_out.at[k],
            dst_ref=edge_in.at[1 - k],
            send_sem=edge_send_sem.at[k],
            recv_sem=edge_recv_sem.at[k],
            device_id=sides[k],
            device_id_type=MESH,
        )
        for k in range(2)
    ]

    @pl.when(my_row == 0)
    def _():
        pl.semaphore_wait(edge_ready.at[0], 1)

    @pl.when(my_row < n_row - 1)
    def _():
        pl.semaphore_wait(edge_ready.at[1], 1)

    for copy in edge_copies:
        copy.start()

    bytes_of(send.at[pl.ds(0, n_grp - 1)], sent).wait_send()

    for copy in edge_copies:
        copy.wait()
    low_ref[...] = edge_in[0]
    high_ref[...] = edge_in[1]


def nodes_kernel(
    elems_total, n_row, tend_ref, low_ref, high_ref, near_ref, out_hbm, done, scratch, sems
):
    fields, _, levels, width = tend_ref.shape
    here = (lax.axis_index("grp") * n_row + lax.axis_index("row")) * width
    elem = lax.broadcasted_iota(jnp.int32, (4, width), 1)
    away = near_ref[...] - (here + elem)
    away = jnp.where(away > elems_total // 2, away - elems_total, away)
    away = jnp.where(away < -(elems_total // 2), away + elems_total, away)
    place = elem + away
    inner = jnp.clip(place, 0, width - 1)
    outer = jnp.clip(jnp.where(place < 0, place + 32, place - width), 0, 31)
    inside = (place >= 0) & (place < width)

    def all_rows(x, k):
        return jnp.broadcast_to(x[k : k + 1], (8, width))

    inner = [all_rows(inner, k) for k in range(4)]
    outer = [all_rows(outer, k) for k in range(4)]
    inside = [all_rows(inside, k) for k in range(4)]

    def pick(values, index):
        return jnp.take_along_axis(values, index, axis=1, mode="promise_in_bounds")

    sub = lax.broadcasted_iota(jnp.int32, (8, width), 0)
    g1 = float(1.0 / np.sqrt(5.0))
    i_of = sub % 4
    g_i = jnp.where(i_of == 0, -1.0, jnp.where(i_of == 1, -g1, jnp.where(i_of == 2, g1, 1.0)))
    west_side = i_of < 2
    g_south = jnp.where(sub < 4, -1.0, -g1)
    g_north = jnp.where(sub < 4, g1, 1.0)

    def write(f):
        return pltpu.make_async_copy(done.at[f], out_hbm.at[f], sems.at[f])

    def field(f, carry):
        shift = 32 * (f // 2)
        for b in range(levels // 8):
            at = slice(8 * b, 8 * b + 8)
            t = [tend_ref[f, c, at, :] for c in range(4)]
            mean = 0.25 * ((t[0] + t[1]) + (t[2] + t[3]))
            halo_at = pl.ds(pl.multiple_of((f % 2) * levels + 8 * b, 8), 8)
            halos = (low_ref[halo_at, :], high_ref[halo_at, :])
            near = []
            for k in range(4):
                if k < 2:
                    own_pick = pltpu.roll(mean, 1 if k == 0 else width - 1, 1)
                else:
                    own_pick = pick(mean, inner[k])
                halo_pick = pick(halos[k % 2], outer[k] + shift)
                near.append(jnp.where(inside[k], own_pick, halo_pick))
            low = functools.reduce(jnp.minimum, t + near)
            high = functools.reduce(jnp.maximum, t + near)
            slope_x = 0.5 * ((t[1] + t[3]) - (t[0] + t[2]))
            slope_y = 0.5 * ((t[2] + t[3]) - (t[0] + t[1]))
            scratch[0, at, :] = mean
            scratch[1, at, :] = slope_x - 0.5 * (near[0] - mean)
            scratch[2, at, :] = slope_x + 0.5 * (near[1] - mean)
            scratch[3, at, :] = slope_y - 0.5 * (near[2] - mean)
            scratch[4, at, :] = slope_y + 0.5 * (near[3] - mean)
            scratch[5, at, :] = (t[3] - t[2]) - (t[1] - t[0])
            scratch[6, at, :] = low
            scratch[7, at, :] = high
        for l in range(levels):
            mean, x_west, x_east, y_south, y_north, cross, low, high = (
                jnp.broadcast_to(scratch[k, l : l + 1, :], (8, width)) for k in range(8)
            )
            base = mean + g_i * jnp.where(west_side, x_west, x_east)
            twist = g_i * cross
            done[f, l, 0:8, :] = jnp.minimum(
                jnp.maximum(base + g_south * (y_south + twist), low), high
            )
            done[f, l, 8:16, :] = jnp.minimum(
                jnp.maximum(base + g_north * (y_north + twist), low), high
            )
        write(f).start()
        return carry

    lax.fori_loop(0, fields, field, 0)
    for f in range(fields):
        write(f).wait()


def on_device(n_grp, n_row, n_x, gll_state, metric, phys_owner, neighbours, rate, forcing, mix):
    fields, levels, nodes, elems = gll_state.shape
    slots, n_z = rate.shape[1], n_grp // n_x
    hbm = pl.BlockSpec(memory_space=pltpu.HBM)
    vmem = pl.BlockSpec(memory_space=pltpu.VMEM)
    tend, low, high = pl.pallas_call(
        functools.partial(exchange_kernel, n_grp, n_row, n_x),
        out_shape=(
            jax.ShapeDtypeStruct((fields, 4, levels, elems), F32),
            jax.ShapeDtypeStruct((2 * levels, elems), F32),
            jax.ShapeDtypeStruct((2 * levels, elems), F32),
        ),
        in_specs=[hbm] * 6,
        out_specs=(vmem, vmem, vmem),
        scratch_shapes=[
            pltpu.VMEM((fields, levels * nodes, elems), F32),
            pltpu.VMEM((nodes, elems), F32),
            pltpu.VMEM((4, elems), jnp.int32),
            pltpu.VMEM((levels, slots), F32),
            pltpu.VMEM((levels, slots), F32),
            pltpu.SMEM((fields, fields), F32),
            pltpu.VMEM((64, elems), F32),
            pltpu.VMEM((slots, 128), F32),
            pltpu.VMEM((n_grp, HIGH, 128), F32),
            pltpu.VMEM((n_grp, HIGH, 128), F32),
            pltpu.VMEM((n_grp * 16, 128), F32),
            pltpu.VMEM((n_grp * 16, 4 * elems), BF16),
            pltpu.VMEM((fields, 4, levels, elems), F32),
            pltpu.VMEM((2, 2 * levels, elems), F32),
            pltpu.VMEM((2, 2 * levels, elems), F32),
            pltpu.SemaphoreType.DMA((6,)),
            pltpu.SemaphoreType.DMA,
            pltpu.SemaphoreType.DMA((n_z,)),
            pltpu.SemaphoreType.DMA((2,)),
            pltpu.SemaphoreType.DMA((2,)),
            pltpu.SemaphoreType.REGULAR((n_z,)),
            pltpu.SemaphoreType.REGULAR((2,)),
        ],
        compiler_params=pltpu.CompilerParams(
            collective_id=0, has_side_effects=True, vmem_limit_bytes=16 << 20
        ),
        name="exchange",
    )(
        *(
            pltpu.with_memory_space_constraint(x, pltpu.HBM)
            for x in (
                gll_state.reshape(fields, levels * nodes, elems),
                metric,
                phys_owner[:, :, 0].T,
                rate,
                forcing,
                mix,
            )
        )
    )
    return pl.pallas_call(
        functools.partial(nodes_kernel, elems * n_grp * n_row, n_row),
        out_shape=jax.ShapeDtypeStruct(gll_state.shape, F32),
        in_specs=[vmem] * 4,
        out_specs=hbm,
        scratch_shapes=[
            pltpu.VMEM((fields, levels, nodes, elems), F32),
            pltpu.VMEM((8, levels, elems), F32),
            pltpu.SemaphoreType.DMA((fields,)),
        ],
        compiler_params=pltpu.CompilerParams(vmem_limit_bytes=16 << 20),
        name="nodes",
    )(tend, low, high, neighbours)


def solution(mesh):
    in_specs = (
        P(None, None, None, ("grp", "row")),
        P(None, ("grp", "row")),
        P(("grp", "row"), None, None),
        P(None, ("grp", "row")),
        P(None, ("grp", "row")),
        P(None, ("grp", "row")),
        P(),
    )
    out_specs = P(None, None, None, ("grp", "row"))
    n_grp, n_row = mesh.shape["grp"], mesh.shape["row"]
    return jax.shard_map(
        functools.partial(on_device, n_grp, n_row, 4),
        mesh=mesh,
        in_specs=in_specs,
        out_specs=out_specs,
        check_vma=False,
    )
```

```python
import functools

import jax
import jax.numpy as jnp
import numpy as np
from jax import lax
from jax.experimental import pallas as pl
from jax.experimental.pallas import tpu as pltpu
from jax.sharding import PartitionSpec as P

MESH = pl.DeviceIdType.MESH
F32 = jnp.float32
BF16 = jnp.bfloat16
HIGH = 11


def lagrange_value(gll_nodes, node_index, point):
    value = 1.0
    for other_index in range(4):
        if other_index != node_index:
            value = (
                value
                * (point - gll_nodes[other_index])
                / (gll_nodes[node_index] - gll_nodes[other_index])
            )
    return value


def cell_weights():
    gll_nodes = np.array([-1.0, -1.0 / np.sqrt(5.0), 1.0 / np.sqrt(5.0), 1.0])
    offset = 0.5 / np.sqrt(3.0)
    halves = np.zeros((2, 4))
    for i in range(4):
        halves[0, i] = 0.5 * (
            lagrange_value(gll_nodes, i, -0.5 - offset)
            + lagrange_value(gll_nodes, i, -0.5 + offset)
        )
        halves[1, i] = 0.5 * (
            lagrange_value(gll_nodes, i, 0.5 - offset) + lagrange_value(gll_nodes, i, 0.5 + offset)
        )
    return (halves[None, :, None, :] * halves[:, None, :, None]).reshape(4, 16)


def exchange_kernel(
    n_grp,
    n_row,
    n_x,
    gll_hbm,
    metric_hbm,
    owner_hbm,
    rate_hbm,
    forcing_hbm,
    mix_hbm,
    tend_ref,
    low_ref,
    high_ref,
    gbuf,
    metric_ref,
    owner_ref,
    rate_ref,
    forcing_ref,
    mix_ref,
    wbuf,
    slots_t,
    send,
    recv,
    rows,
    onehot,
    cells,
    edge_out,
    edge_in,
    in_sem,
    sent,
    came,
    edge_send_sem,
    edge_recv_sem,
    ready,
    edge_ready,
):
    fields = gll_hbm.shape[0]
    me = lax.axis_index("grp")
    my_row = lax.axis_index("row")
    n_z = n_grp // n_x
    my_z, my_x = me // n_x, me % n_x
    around = [(my_x + d) % n_x for d in (2, 1, 3, 0)]

    small = [
        pltpu.make_async_copy(src, dst, in_sem.at[k])
        for k, (src, dst) in enumerate(
            (
                (rate_hbm, rate_ref),
                (forcing_hbm, forcing_ref),
                (metric_hbm, metric_ref),
                (owner_hbm, owner_ref),
                (mix_hbm, mix_ref),
            )
        )
    ]
    for copy in small[:2]:
        copy.start()
    gll_copy = pltpu.make_async_copy(gll_hbm, gbuf, in_sem.at[5])
    here = me * n_row + my_row
    total = n_grp * n_row
    after = lax.rem(here + 1, total)
    before = lax.rem(here + total - 1, total)
    sides = [(d // n_row, d % n_row) for d in (before, after)]

    barrier = pltpu.get_barrier_semaphore()

    def greet(g, carry):
        pl.semaphore_signal(barrier, inc=1, device_id=(g, my_row), device_id_type=MESH)
        return carry

    lax.fori_loop(me + 1, n_grp, greet, 0)

    @pl.when(my_row < n_row - 1)
    def _():
        pl.semaphore_signal(barrier, inc=1, device_id=sides[1], device_id_type=MESH)

    @pl.when(my_row == 0)
    def _():
        pl.semaphore_signal(barrier, inc=1, device_id=sides[0], device_id_type=MESH)

    beside = jnp.where(my_row > 0, 1, 0) + jnp.where(my_row == n_row - 1, 1, 0)

    small[0].wait()
    small[1].wait()
    for copy in small[2:]:
        copy.start()
    gll_copy.start()
    slot_count = rate_ref.shape[1]
    for k in range(0, slot_count, 128):
        width = min(128, slot_count - k)
        r = rate_ref[:, k : k + width]
        f = forcing_ref[:, k : k + width]
        slots_t[k : k + width, :] = jnp.concatenate([r, f, r, f], axis=0).T
    lane = lax.broadcasted_iota(jnp.int32, (HIGH, 128), 1)
    for g in range(n_grp):
        at = 2 * HIGH * g
        send[g] = jnp.where(lane < 64, slots_t[at : at + HIGH], slots_t[at + HIGH : at + 2 * HIGH])

    @pl.when(here > 0)
    def _():
        pl.semaphore_wait(barrier, me + beside)

    @pl.when(my_row > 0)
    def _():
        pl.semaphore_signal(edge_ready.at[1], inc=1, device_id=sides[0], device_id_type=MESH)

    @pl.when(my_row == n_row - 1)
    def _():
        pl.semaphore_signal(edge_ready.at[0], inc=1, device_id=sides[1], device_id_type=MESH)

    def block_copy(there, origin):
        return pltpu.make_async_remote_copy(
            src_ref=send.at[there],
            dst_ref=recv.at[me],
            send_sem=sent,
            recv_sem=came.at[origin],
            device_id=(there, my_row),
            device_id_type=MESH,
        )

    def tell(g):
        pl.semaphore_signal(ready.at[my_z], inc=1, device_id=(g, my_row), device_id_type=MESH)

    def send_down(z, carry):
        for x in around:
            tell(z * n_x + x)
            block_copy(z * n_x + x, my_z).start()
        return carry

    lax.fori_loop(0, my_z, send_down, 0)

    def send_beside(g, carry):
        tell(g)
        block_copy(g, my_z).start()
        return carry

    lax.fori_loop(my_z * n_x, me, send_beside, 0)

    small[2].wait()
    table = cell_weights()
    for c in range(4):
        weighted = [metric_ref[n : n + 1, :] * float(table[c, n]) for n in range(16)]
        area = functools.reduce(lambda a, b: a + b, weighted)
        inverse = 1.0 / area
        for n in range(16):
            wbuf[16 * c + n : 16 * c + n + 1, :] = weighted[n] * inverse

    levels = tend_ref.shape[2]
    gll_copy.wait()

    def to_cells(f, carry):
        sums = [None] * 4
        for n in range(16):
            g = gbuf[f, pl.ds(n, levels, stride=16), :]
            for c in range(4):
                term = wbuf[16 * c + n : 16 * c + n + 1, :] * g
                sums[c] = term if sums[c] is None else sums[c] + term
        for c in range(4):
            cells[f, c] = sums[c]
        return carry

    lax.fori_loop(0, fields // 2, to_cells, 0)
    lax.fori_loop(fields // 2, fields, to_cells, 0)

    small[4].wait()

    def mix(i, carry):
        c, at = i // (levels // 8), pl.multiple_of((i % (levels // 8)) * 8, 8)
        block = [cells[g, c, pl.ds(at, 8), :] for g in range(fields)]
        for f in range(fields):
            total_f = mix_ref[f, 0] * block[0]
            for g in range(1, fields):
                total_f = total_f + mix_ref[f, g] * block[g]
            cells[f, c, pl.ds(at, 8), :] = total_f
        return carry

    lax.fori_loop(0, 4 * (levels // 8), mix, 0)

    small[3].wait()
    grp_ids = lax.broadcasted_iota(jnp.int32, (n_grp, 128), 0)
    owners = [owner_ref[c : c + 1, :] for c in range(4)]
    match = [jnp.where(grp_ids == owners[c], 1.0, 0.0).astype(F32) for c in range(4)]
    count = match[0] + match[1] + match[2] + match[3]
    before_e = lax.broadcasted_iota(jnp.int32, (128, 128), 0) < lax.broadcasted_iota(
        jnp.int32, (128, 128), 1
    )
    running = jnp.dot(
        count.astype(BF16),
        jnp.where(before_e, 1.0, 0.0).astype(BF16),
        preferred_element_type=F32,
    )
    upper = []
    row_ids = lax.broadcasted_iota(jnp.int32, (256, 128), 0)
    for c in range(4):
        rank = jnp.sum(match[c] * running, axis=0, keepdims=True).astype(jnp.int32)
        running = running + match[c]
        is_upper = rank >= HIGH
        upper.append(is_upper)
        key = owners[c] * 16 + jnp.where(is_upper, rank - HIGH, rank)
        for k in range(n_grp * 16 // 256):
            onehot[256 * k : 256 * k + 256, 128 * c : 128 * c + 128] = jnp.where(
                row_ids == key - 256 * k, 1.0, 0.0
            ).astype(BF16)

    rows[...] = jnp.zeros_like(rows)
    recv[me] = send[me]

    @pl.when(my_x < n_x - 1)
    def _():
        pl.semaphore_wait(ready.at[my_z], n_x - 1 - my_x)

    def start_up(g, carry):
        block_copy(g, my_z).start()
        return carry

    lax.fori_loop(me + 1, (my_z + 1) * n_x, start_up, 0)

    def send_up(z, carry):
        pl.semaphore_wait(ready.at[z], n_x)
        for x in around:
            block_copy(z * n_x + x, my_z).start()
        return carry

    lax.fori_loop(my_z + 1, n_z, send_up, 0)

    def bytes_of(what, sem):
        return pltpu.make_async_remote_copy(
            src_ref=what,
            dst_ref=what,
            send_sem=sem,
            recv_sem=sem,
            device_id=sides[0],
            device_id_type=MESH,
        )

    picked = None
    for k in range(n_z // 4):
        for z in range(4 * k, 4 * k + 4):

            @pl.when(z != my_z)
            def _():
                bytes_of(recv.at[pl.ds(0, n_x)], came.at[z]).wait_recv()

            @pl.when(z == my_z)
            def _():
                bytes_of(recv.at[pl.ds(0, n_x - 1)], came.at[z]).wait_recv()

        for g in range(16 * k, 16 * k + 16):
            rows[16 * g : 16 * g + HIGH, :] = recv[g]
        block = rows[256 * k : 256 * k + 256, :].T
        top = block.astype(BF16)
        rest = (block - top.astype(F32)).astype(BF16)
        hot = onehot[256 * k : 256 * k + 256, :]
        part = jnp.dot(top, hot, preferred_element_type=F32) + jnp.dot(
            rest, hot, preferred_element_type=F32
        )
        picked = part if picked is None else picked + part

    for c in range(4):
        cut = picked[:, 128 * c : 128 * c + 128]
        both = jnp.where(upper[c], cut[64:128], cut[0:64])
        for f in range(fields):
            tend_ref[f, c] = both[:levels] * jnp.tanh(cells[f, c] + both[levels:])

    lanes = lax.broadcasted_iota(jnp.int32, (levels, 128), 1)
    for half in range(2):
        first, last = None, None
        for q in range(fields // 2):
            f = 2 * q + half
            mean = 0.25 * ((tend_ref[f, 0] + tend_ref[f, 1]) + (tend_ref[f, 2] + tend_ref[f, 3]))
            inside = (lanes >= 32 * q) & (lanes < 32 * q + 32)
            low = pltpu.roll(mean, 32 * q, 1) if q else mean
            high = pltpu.roll(mean, (32 * q + 32) % 128, 1) if (32 * q + 32) % 128 else mean
            first = low if first is None else jnp.where(inside, low, first)
            last = high if last is None else jnp.where(inside, high, last)
        edge_out[0, half * levels : half * levels + levels, :] = first
        edge_out[1, half * levels : half * levels + levels, :] = last

    edge_copies = [
        pltpu.make_async_remote_copy(
            src_ref=edge_out.at[k],
            dst_ref=edge_in.at[1 - k],
            send_sem=edge_send_sem.at[k],
            recv_sem=edge_recv_sem.at[k],
            device_id=sides[k],
            device_id_type=MESH,
        )
        for k in range(2)
    ]

    @pl.when(my_row == 0)
    def _():
        pl.semaphore_wait(edge_ready.at[0], 1)

    @pl.when(my_row < n_row - 1)
    def _():
        pl.semaphore_wait(edge_ready.at[1], 1)

    for copy in edge_copies:
        copy.start()

    bytes_of(send.at[pl.ds(0, n_grp - 1)], sent).wait_send()

    for copy in edge_copies:
        copy.wait()
    low_ref[...] = edge_in[0]
    high_ref[...] = edge_in[1]


def nodes_kernel(
    elems_total, n_row, tend_ref, low_ref, high_ref, near_ref, out_hbm, done, scratch, sem
):
    fields, _, levels, width = tend_ref.shape
    here = (lax.axis_index("grp") * n_row + lax.axis_index("row")) * width
    elem = lax.broadcasted_iota(jnp.int32, (4, width), 1)
    away = near_ref[...] - (here + elem)
    away = jnp.where(away > elems_total // 2, away - elems_total, away)
    away = jnp.where(away < -(elems_total // 2), away + elems_total, away)
    place = elem + away
    inner = jnp.clip(place, 0, width - 1)
    outer = jnp.clip(jnp.where(place < 0, place + 32, place - width), 0, 31)
    inside = (place >= 0) & (place < width)

    def all_rows(x, k):
        return jnp.broadcast_to(x[k : k + 1], (8, width))

    inner = [all_rows(inner, k) for k in range(4)]
    outer = [all_rows(outer, k) for k in range(4)]
    inside = [all_rows(inside, k) for k in range(4)]

    def pick(values, index):
        return jnp.take_along_axis(values, index, axis=1, mode="promise_in_bounds")

    sub = lax.broadcasted_iota(jnp.int32, (8, width), 0)
    g1 = float(1.0 / np.sqrt(5.0))
    i_of = sub % 4
    g_i = jnp.where(i_of == 0, -1.0, jnp.where(i_of == 1, -g1, jnp.where(i_of == 2, g1, 1.0)))
    west_side = i_of < 2
    g_south = jnp.where(sub < 4, -1.0, -g1)
    g_north = jnp.where(sub < 4, g1, 1.0)

    def write(f):
        return pltpu.make_async_copy(done.at[f], out_hbm.at[f], sem)

    def field(f, carry):
        shift = 32 * (f // 2)
        for b in range(levels // 8):
            at = slice(8 * b, 8 * b + 8)
            t = [tend_ref[f, c, at, :] for c in range(4)]
            mean = 0.25 * ((t[0] + t[1]) + (t[2] + t[3]))
            halo_at = pl.ds(pl.multiple_of((f % 2) * levels + 8 * b, 8), 8)
            halos = (low_ref[halo_at, :], high_ref[halo_at, :])
            near = []
            for k in range(4):
                if k < 2:
                    own_pick = pltpu.roll(mean, 1 if k == 0 else width - 1, 1)
                else:
                    own_pick = pick(mean, inner[k])
                halo_pick = pick(halos[k % 2], outer[k] + shift)
                near.append(jnp.where(inside[k], own_pick, halo_pick))
            low = functools.reduce(jnp.minimum, t + near)
            high = functools.reduce(jnp.maximum, t + near)
            slope_x = 0.5 * ((t[1] + t[3]) - (t[0] + t[2]))
            slope_y = 0.5 * ((t[2] + t[3]) - (t[0] + t[1]))
            scratch[0, at, :] = mean
            scratch[1, at, :] = slope_x - 0.5 * (near[0] - mean)
            scratch[2, at, :] = slope_x + 0.5 * (near[1] - mean)
            scratch[3, at, :] = slope_y - 0.5 * (near[2] - mean)
            scratch[4, at, :] = slope_y + 0.5 * (near[3] - mean)
            scratch[5, at, :] = (t[3] - t[2]) - (t[1] - t[0])
            scratch[6, at, :] = low
            scratch[7, at, :] = high
        for l in range(levels):
            mean, x_west, x_east, y_south, y_north, cross, low, high = (
                jnp.broadcast_to(scratch[k, l : l + 1, :], (8, width)) for k in range(8)
            )
            base = mean + g_i * jnp.where(west_side, x_west, x_east)
            twist = g_i * cross
            done[f, l, 0:8, :] = jnp.minimum(
                jnp.maximum(base + g_south * (y_south + twist), low), high
            )
            done[f, l, 8:16, :] = jnp.minimum(
                jnp.maximum(base + g_north * (y_north + twist), low), high
            )
        write(f).start()
        return carry

    lax.fori_loop(0, fields, field, 0)
    pltpu.make_async_copy(done, out_hbm, sem).wait()


def on_device(n_grp, n_row, n_x, gll_state, metric, phys_owner, neighbours, rate, forcing, mix):
    fields, levels, nodes, elems = gll_state.shape
    slots, n_z = rate.shape[1], n_grp // n_x
    hbm = pl.BlockSpec(memory_space=pltpu.HBM)
    vmem = pl.BlockSpec(memory_space=pltpu.VMEM)
    tend, low, high = pl.pallas_call(
        functools.partial(exchange_kernel, n_grp, n_row, n_x),
        out_shape=(
            jax.ShapeDtypeStruct((fields, 4, levels, elems), F32),
            jax.ShapeDtypeStruct((2 * levels, elems), F32),
            jax.ShapeDtypeStruct((2 * levels, elems), F32),
        ),
        in_specs=[hbm] * 6,
        out_specs=(vmem, vmem, vmem),
        scratch_shapes=[
            pltpu.VMEM((fields, levels * nodes, elems), F32),
            pltpu.VMEM((nodes, elems), F32),
            pltpu.VMEM((4, elems), jnp.int32),
            pltpu.VMEM((levels, slots), F32),
            pltpu.VMEM((levels, slots), F32),
            pltpu.SMEM((fields, fields), F32),
            pltpu.VMEM((64, elems), F32),
            pltpu.VMEM((slots, 128), F32),
            pltpu.VMEM((n_grp, HIGH, 128), F32),
            pltpu.VMEM((n_grp, HIGH, 128), F32),
            pltpu.VMEM((n_grp * 16, 128), F32),
            pltpu.VMEM((n_grp * 16, 4 * elems), BF16),
            pltpu.VMEM((fields, 4, levels, elems), F32),
            pltpu.VMEM((2, 2 * levels, elems), F32),
            pltpu.VMEM((2, 2 * levels, elems), F32),
            pltpu.SemaphoreType.DMA((6,)),
            pltpu.SemaphoreType.DMA,
            pltpu.SemaphoreType.DMA((n_z,)),
            pltpu.SemaphoreType.DMA((2,)),
            pltpu.SemaphoreType.DMA((2,)),
            pltpu.SemaphoreType.REGULAR((n_z,)),
            pltpu.SemaphoreType.REGULAR((2,)),
        ],
        compiler_params=pltpu.CompilerParams(
            collective_id=0, has_side_effects=True, vmem_limit_bytes=16 << 20
        ),
        name="exchange",
    )(
        *(
            pltpu.with_memory_space_constraint(x, pltpu.HBM)
            for x in (
                gll_state.reshape(fields, levels * nodes, elems),
                metric,
                phys_owner[:, :, 0].T,
                rate,
                forcing,
                mix,
            )
        )
    )
    return pl.pallas_call(
        functools.partial(nodes_kernel, elems * n_grp * n_row, n_row),
        out_shape=jax.ShapeDtypeStruct(gll_state.shape, F32),
        in_specs=[vmem] * 4,
        out_specs=hbm,
        scratch_shapes=[
            pltpu.VMEM((fields, levels, nodes, elems), F32),
            pltpu.VMEM((8, levels, elems), F32),
            pltpu.SemaphoreType.DMA,
        ],
        compiler_params=pltpu.CompilerParams(vmem_limit_bytes=16 << 20),
        name="nodes",
    )(tend, low, high, neighbours)


def solution(mesh):
    in_specs = (
        P(None, None, None, ("grp", "row")),
        P(None, ("grp", "row")),
        P(("grp", "row"), None, None),
        P(None, ("grp", "row")),
        P(None, ("grp", "row")),
        P(None, ("grp", "row")),
        P(),
    )
    out_specs = P(None, None, None, ("grp", "row"))
    n_grp, n_row = mesh.shape["grp"], mesh.shape["row"]
    return jax.shard_map(
        functools.partial(on_device, n_grp, n_row, 4),
        mesh=mesh,
        in_specs=in_specs,
        out_specs=out_specs,
        check_vma=False,
    )
```

```python
import functools

import jax
import jax.numpy as jnp
import numpy as np
from jax import lax
from jax.experimental import pallas as pl
from jax.experimental.pallas import tpu as pltpu
from jax.sharding import PartitionSpec as P

MESH = pl.DeviceIdType.MESH
F32 = jnp.float32
BF16 = jnp.bfloat16
HIGH = 11


def lagrange_value(gll_nodes, node_index, point):
    value = 1.0
    for other_index in range(4):
        if other_index != node_index:
            value = (
                value
                * (point - gll_nodes[other_index])
                / (gll_nodes[node_index] - gll_nodes[other_index])
            )
    return value


def cell_weights():
    gll_nodes = np.array([-1.0, -1.0 / np.sqrt(5.0), 1.0 / np.sqrt(5.0), 1.0])
    offset = 0.5 / np.sqrt(3.0)
    halves = np.zeros((2, 4))
    for i in range(4):
        halves[0, i] = 0.5 * (
            lagrange_value(gll_nodes, i, -0.5 - offset)
            + lagrange_value(gll_nodes, i, -0.5 + offset)
        )
        halves[1, i] = 0.5 * (
            lagrange_value(gll_nodes, i, 0.5 - offset) + lagrange_value(gll_nodes, i, 0.5 + offset)
        )
    return (halves[None, :, None, :] * halves[:, None, :, None]).reshape(4, 16)


def exchange_kernel(
    n_grp,
    n_row,
    n_x,
    gll_hbm,
    metric_hbm,
    owner_hbm,
    rate_hbm,
    forcing_hbm,
    mix_hbm,
    tend_ref,
    low_ref,
    high_ref,
    gbuf,
    metric_ref,
    owner_ref,
    rate_ref,
    forcing_ref,
    mix_ref,
    wbuf,
    slots_t,
    send,
    recv,
    rows,
    onehot,
    cells,
    edge_out,
    edge_in,
    in_sem,
    sent,
    came,
    edge_send_sem,
    edge_recv_sem,
    ready,
    edge_ready,
):
    fields = gll_hbm.shape[0]
    me = lax.axis_index("grp")
    my_row = lax.axis_index("row")
    n_z = n_grp // n_x
    my_z, my_x = me // n_x, me % n_x
    around = [(my_x + d) % n_x for d in (2, 1, 3, 0)]

    small = [
        pltpu.make_async_copy(src, dst, in_sem.at[k])
        for k, (src, dst) in enumerate(
            (
                (rate_hbm, rate_ref),
                (forcing_hbm, forcing_ref),
                (metric_hbm, metric_ref),
                (owner_hbm, owner_ref),
                (mix_hbm, mix_ref),
            )
        )
    ]
    for copy in small[:2]:
        copy.start()
    gll_copy = pltpu.make_async_copy(gll_hbm, gbuf, in_sem.at[5])
    here = me * n_row + my_row
    total = n_grp * n_row
    after = lax.rem(here + 1, total)
    before = lax.rem(here + total - 1, total)
    sides = [(d // n_row, d % n_row) for d in (before, after)]

    barrier = pltpu.get_barrier_semaphore()

    def greet(g, carry):
        pl.semaphore_signal(barrier, inc=1, device_id=(g, my_row), device_id_type=MESH)
        return carry

    lax.fori_loop(me + 1, n_grp, greet, 0)

    @pl.when(my_row < n_row - 1)
    def _():
        pl.semaphore_signal(barrier, inc=1, device_id=sides[1], device_id_type=MESH)

    @pl.when(my_row == 0)
    def _():
        pl.semaphore_signal(barrier, inc=1, device_id=sides[0], device_id_type=MESH)

    beside = jnp.where(my_row > 0, 1, 0) + jnp.where(my_row == n_row - 1, 1, 0)

    small[0].wait()
    small[1].wait()
    for copy in small[2:]:
        copy.start()
    gll_copy.start()
    slot_count = rate_ref.shape[1]
    for k in range(0, slot_count, 128):
        width = min(128, slot_count - k)
        r = rate_ref[:, k : k + width]
        f = forcing_ref[:, k : k + width]
        slots_t[k : k + width, :] = jnp.concatenate([r, f, r, f], axis=0).T
    lane = lax.broadcasted_iota(jnp.int32, (HIGH, 128), 1)
    for g in range(n_grp):
        at = 2 * HIGH * g
        send[g] = jnp.where(lane < 64, slots_t[at : at + HIGH], slots_t[at + HIGH : at + 2 * HIGH])

    @pl.when(here > 0)
    def _():
        pl.semaphore_wait(barrier, me + beside)

    @pl.when(my_row > 0)
    def _():
        pl.semaphore_signal(edge_ready.at[1], inc=1, device_id=sides[0], device_id_type=MESH)

    @pl.when(my_row == n_row - 1)
    def _():
        pl.semaphore_signal(edge_ready.at[0], inc=1, device_id=sides[1], device_id_type=MESH)

    def block_copy(there, origin):
        return pltpu.make_async_remote_copy(
            src_ref=send.at[there],
            dst_ref=recv.at[me],
            send_sem=sent,
            recv_sem=came.at[origin],
            device_id=(there, my_row),
            device_id_type=MESH,
        )

    def tell(g):
        pl.semaphore_signal(ready.at[my_z], inc=1, device_id=(g, my_row), device_id_type=MESH)

    def send_down(z, carry):
        for x in around:
            tell(z * n_x + x)
            block_copy(z * n_x + x, my_z).start()
        return carry

    lax.fori_loop(0, my_z, send_down, 0)

    def send_beside(g, carry):
        tell(g)
        block_copy(g, my_z).start()
        return carry

    lax.fori_loop(my_z * n_x, me, send_beside, 0)

    small[2].wait()
    table = cell_weights()
    for c in range(4):
        weighted = [metric_ref[n : n + 1, :] * float(table[c, n]) for n in range(16)]
        area = functools.reduce(lambda a, b: a + b, weighted)
        inverse = 1.0 / area
        for n in range(16):
            wbuf[16 * c + n : 16 * c + n + 1, :] = weighted[n] * inverse

    levels = tend_ref.shape[2]
    gll_copy.wait()

    def to_cells(f, carry):
        sums = [None] * 4
        for n in range(16):
            g = gbuf[f, pl.ds(n, levels, stride=16), :]
            for c in range(4):
                term = wbuf[16 * c + n : 16 * c + n + 1, :] * g
                sums[c] = term if sums[c] is None else sums[c] + term
        for c in range(4):
            cells[f, c] = sums[c]
        return carry

    lax.fori_loop(0, fields // 2, to_cells, 0)
    lax.fori_loop(fields // 2, fields, to_cells, 0)

    small[4].wait()

    def mix(i, carry):
        c, at = i // (levels // 8), pl.multiple_of((i % (levels // 8)) * 8, 8)
        block = [cells[g, c, pl.ds(at, 8), :] for g in range(fields)]
        for f in range(fields):
            total_f = mix_ref[f, 0] * block[0]
            for g in range(1, fields):
                total_f = total_f + mix_ref[f, g] * block[g]
            cells[f, c, pl.ds(at, 8), :] = total_f
        return carry

    lax.fori_loop(0, 4 * (levels // 8), mix, 0)

    small[3].wait()
    grp_ids = lax.broadcasted_iota(jnp.int32, (n_grp, 128), 0)
    owners = [owner_ref[c : c + 1, :] for c in range(4)]
    match = [jnp.where(grp_ids == owners[c], 1.0, 0.0).astype(F32) for c in range(4)]
    count = match[0] + match[1] + match[2] + match[3]
    before_e = lax.broadcasted_iota(jnp.int32, (128, 128), 0) < lax.broadcasted_iota(
        jnp.int32, (128, 128), 1
    )
    running = jnp.dot(
        count.astype(BF16),
        jnp.where(before_e, 1.0, 0.0).astype(BF16),
        preferred_element_type=F32,
    )
    upper = []
    row_ids = lax.broadcasted_iota(jnp.int32, (256, 128), 0)
    for c in range(4):
        rank = jnp.sum(match[c] * running, axis=0, keepdims=True).astype(jnp.int32)
        running = running + match[c]
        is_upper = rank >= HIGH
        upper.append(is_upper)
        key = owners[c] * 16 + jnp.where(is_upper, rank - HIGH, rank)
        for k in range(n_grp * 16 // 256):
            onehot[256 * k : 256 * k + 256, 128 * c : 128 * c + 128] = jnp.where(
                row_ids == key - 256 * k, 1.0, 0.0
            ).astype(BF16)

    rows[...] = jnp.zeros_like(rows)
    recv[me] = send[me]

    @pl.when(my_x < n_x - 1)
    def _():
        pl.semaphore_wait(ready.at[my_z], n_x - 1 - my_x)

    def start_up(g, carry):
        block_copy(g, my_z).start()
        return carry

    lax.fori_loop(me + 1, (my_z + 1) * n_x, start_up, 0)

    def send_up(z, carry):
        pl.semaphore_wait(ready.at[z], n_x)
        for x in around:
            block_copy(z * n_x + x, my_z).start()
        return carry

    lax.fori_loop(my_z + 1, n_z, send_up, 0)

    def bytes_of(what, sem):
        return pltpu.make_async_remote_copy(
            src_ref=what,
            dst_ref=what,
            send_sem=sem,
            recv_sem=sem,
            device_id=sides[0],
            device_id_type=MESH,
        )

    picked = None
    for k in range(n_z // 4):
        for z in range(4 * k, 4 * k + 4):

            @pl.when(z != my_z)
            def _():
                bytes_of(recv.at[pl.ds(0, n_x)], came.at[z]).wait_recv()

            @pl.when(z == my_z)
            def _():
                bytes_of(recv.at[pl.ds(0, n_x - 1)], came.at[z]).wait_recv()

        for g in range(16 * k, 16 * k + 16):
            rows[16 * g : 16 * g + HIGH, :] = recv[g]
        block = rows[256 * k : 256 * k + 256, :].T
        top = block.astype(BF16)
        rest = (block - top.astype(F32)).astype(BF16)
        hot = onehot[256 * k : 256 * k + 256, :]
        part = jnp.dot(top, hot, preferred_element_type=F32) + jnp.dot(
            rest, hot, preferred_element_type=F32
        )
        picked = part if picked is None else picked + part

    for c in range(4):
        cut = picked[:, 128 * c : 128 * c + 128]
        both = jnp.where(upper[c], cut[64:128], cut[0:64])
        for f in range(fields):
            tend_ref[f, c] = both[:levels] * jnp.tanh(cells[f, c] + both[levels:])

    lanes = lax.broadcasted_iota(jnp.int32, (levels, 128), 1)
    for half in range(2):
        first, last = None, None
        for q in range(fields // 2):
            f = 2 * q + half
            mean = 0.25 * ((tend_ref[f, 0] + tend_ref[f, 1]) + (tend_ref[f, 2] + tend_ref[f, 3]))
            inside = (lanes >= 32 * q) & (lanes < 32 * q + 32)
            low = pltpu.roll(mean, 32 * q, 1) if q else mean
            high = pltpu.roll(mean, (32 * q + 32) % 128, 1) if (32 * q + 32) % 128 else mean
            first = low if first is None else jnp.where(inside, low, first)
            last = high if last is None else jnp.where(inside, high, last)
        edge_out[0, half * levels : half * levels + levels, :] = first
        edge_out[1, half * levels : half * levels + levels, :] = last

    edge_copies = [
        pltpu.make_async_remote_copy(
            src_ref=edge_out.at[k],
            dst_ref=edge_in.at[1 - k],
            send_sem=edge_send_sem.at[k],
            recv_sem=edge_recv_sem.at[k],
            device_id=sides[k],
            device_id_type=MESH,
        )
        for k in range(2)
    ]

    @pl.when(my_row == 0)
    def _():
        pl.semaphore_wait(edge_ready.at[0], 1)

    @pl.when(my_row < n_row - 1)
    def _():
        pl.semaphore_wait(edge_ready.at[1], 1)

    for copy in edge_copies:
        copy.start()

    bytes_of(send.at[pl.ds(0, n_grp - 1)], sent).wait_send()

    for copy in edge_copies:
        copy.wait()
    low_ref[...] = edge_in[0]
    high_ref[...] = edge_in[1]


def nodes_kernel(
    elems_total, n_row, tend_ref, low_ref, high_ref, near_ref, out_hbm, done, scratch, sem
):
    fields, _, levels, width = tend_ref.shape
    here = (lax.axis_index("grp") * n_row + lax.axis_index("row")) * width
    elem = lax.broadcasted_iota(jnp.int32, (4, width), 1)
    away = near_ref[...] - (here + elem)
    away = jnp.where(away > elems_total // 2, away - elems_total, away)
    away = jnp.where(away < -(elems_total // 2), away + elems_total, away)
    place = elem + away
    inner = jnp.clip(place, 0, width - 1)
    outer = jnp.clip(jnp.where(place < 0, place + 32, place - width), 0, 31)
    inside = (place >= 0) & (place < width)

    def all_rows(x, k):
        return jnp.broadcast_to(x[k : k + 1], (8, width))

    inner = [all_rows(inner, k) for k in range(4)]
    outer = [all_rows(outer, k) for k in range(4)]
    inside = [all_rows(inside, k) for k in range(4)]

    def pick(values, index):
        return jnp.take_along_axis(values, index, axis=1, mode="promise_in_bounds")

    sub = lax.broadcasted_iota(jnp.int32, (8, width), 0)
    g1 = float(1.0 / np.sqrt(5.0))
    i_of = sub % 4
    g_i = jnp.where(i_of == 0, -1.0, jnp.where(i_of == 1, -g1, jnp.where(i_of == 2, g1, 1.0)))
    west_side = i_of < 2
    g_south = jnp.where(sub < 4, -1.0, -g1)
    g_north = jnp.where(sub < 4, g1, 1.0)

    half = levels // 2

    def write(f, k):
        part = pl.ds(half * k, half)
        return pltpu.make_async_copy(done.at[f, part], out_hbm.at[f, part], sem)

    def field(f, carry):
        shift = 32 * (f // 2)
        for b in range(levels // 8):
            at = slice(8 * b, 8 * b + 8)
            t = [tend_ref[f, c, at, :] for c in range(4)]
            mean = 0.25 * ((t[0] + t[1]) + (t[2] + t[3]))
            halo_at = pl.ds(pl.multiple_of((f % 2) * levels + 8 * b, 8), 8)
            halos = (low_ref[halo_at, :], high_ref[halo_at, :])
            near = []
            for k in range(4):
                if k < 2:
                    own_pick = pltpu.roll(mean, 1 if k == 0 else width - 1, 1)
                else:
                    own_pick = pick(mean, inner[k])
                halo_pick = pick(halos[k % 2], outer[k] + shift)
                near.append(jnp.where(inside[k], own_pick, halo_pick))
            low = functools.reduce(jnp.minimum, t + near)
            high = functools.reduce(jnp.maximum, t + near)
            slope_x = 0.5 * ((t[1] + t[3]) - (t[0] + t[2]))
            slope_y = 0.5 * ((t[2] + t[3]) - (t[0] + t[1]))
            scratch[0, at, :] = mean
            scratch[1, at, :] = slope_x - 0.5 * (near[0] - mean)
            scratch[2, at, :] = slope_x + 0.5 * (near[1] - mean)
            scratch[3, at, :] = slope_y - 0.5 * (near[2] - mean)
            scratch[4, at, :] = slope_y + 0.5 * (near[3] - mean)
            scratch[5, at, :] = (t[3] - t[2]) - (t[1] - t[0])
            scratch[6, at, :] = low
            scratch[7, at, :] = high
        for l in range(levels):
            mean, x_west, x_east, y_south, y_north, cross, low, high = (
                jnp.broadcast_to(scratch[k, l : l + 1, :], (8, width)) for k in range(8)
            )
            base = mean + g_i * jnp.where(west_side, x_west, x_east)
            twist = g_i * cross
            done[f, l, 0:8, :] = jnp.minimum(
                jnp.maximum(base + g_south * (y_south + twist), low), high
            )
            done[f, l, 8:16, :] = jnp.minimum(
                jnp.maximum(base + g_north * (y_north + twist), low), high
            )
            if l % half == half - 1:
                write(f, l // half).start()
        return carry

    lax.fori_loop(0, fields, field, 0)
    pltpu.make_async_copy(done, out_hbm, sem).wait()


def on_device(n_grp, n_row, n_x, gll_state, metric, phys_owner, neighbours, rate, forcing, mix):
    fields, levels, nodes, elems = gll_state.shape
    slots, n_z = rate.shape[1], n_grp // n_x
    hbm = pl.BlockSpec(memory_space=pltpu.HBM)
    vmem = pl.BlockSpec(memory_space=pltpu.VMEM)
    tend, low, high = pl.pallas_call(
        functools.partial(exchange_kernel, n_grp, n_row, n_x),
        out_shape=(
            jax.ShapeDtypeStruct((fields, 4, levels, elems), F32),
            jax.ShapeDtypeStruct((2 * levels, elems), F32),
            jax.ShapeDtypeStruct((2 * levels, elems), F32),
        ),
        in_specs=[hbm] * 6,
        out_specs=(vmem, vmem, vmem),
        scratch_shapes=[
            pltpu.VMEM((fields, levels * nodes, elems), F32),
            pltpu.VMEM((nodes, elems), F32),
            pltpu.VMEM((4, elems), jnp.int32),
            pltpu.VMEM((levels, slots), F32),
            pltpu.VMEM((levels, slots), F32),
            pltpu.SMEM((fields, fields), F32),
            pltpu.VMEM((64, elems), F32),
            pltpu.VMEM((slots, 128), F32),
            pltpu.VMEM((n_grp, HIGH, 128), F32),
            pltpu.VMEM((n_grp, HIGH, 128), F32),
            pltpu.VMEM((n_grp * 16, 128), F32),
            pltpu.VMEM((n_grp * 16, 4 * elems), BF16),
            pltpu.VMEM((fields, 4, levels, elems), F32),
            pltpu.VMEM((2, 2 * levels, elems), F32),
            pltpu.VMEM((2, 2 * levels, elems), F32),
            pltpu.SemaphoreType.DMA((6,)),
            pltpu.SemaphoreType.DMA,
            pltpu.SemaphoreType.DMA((n_z,)),
            pltpu.SemaphoreType.DMA((2,)),
            pltpu.SemaphoreType.DMA((2,)),
            pltpu.SemaphoreType.REGULAR((n_z,)),
            pltpu.SemaphoreType.REGULAR((2,)),
        ],
        compiler_params=pltpu.CompilerParams(
            collective_id=0, has_side_effects=True, vmem_limit_bytes=16 << 20
        ),
        name="exchange",
    )(
        *(
            pltpu.with_memory_space_constraint(x, pltpu.HBM)
            for x in (
                gll_state.reshape(fields, levels * nodes, elems),
                metric,
                phys_owner[:, :, 0].T,
                rate,
                forcing,
                mix,
            )
        )
    )
    return pl.pallas_call(
        functools.partial(nodes_kernel, elems * n_grp * n_row, n_row),
        out_shape=jax.ShapeDtypeStruct(gll_state.shape, F32),
        in_specs=[vmem] * 4,
        out_specs=hbm,
        scratch_shapes=[
            pltpu.VMEM((fields, levels, nodes, elems), F32),
            pltpu.VMEM((8, levels, elems), F32),
            pltpu.SemaphoreType.DMA,
        ],
        compiler_params=pltpu.CompilerParams(vmem_limit_bytes=16 << 20),
        name="nodes",
    )(tend, low, high, neighbours)


def solution(mesh):
    in_specs = (
        P(None, None, None, ("grp", "row")),
        P(None, ("grp", "row")),
        P(("grp", "row"), None, None),
        P(None, ("grp", "row")),
        P(None, ("grp", "row")),
        P(None, ("grp", "row")),
        P(),
    )
    out_specs = P(None, None, None, ("grp", "row"))
    n_grp, n_row = mesh.shape["grp"], mesh.shape["row"]
    return jax.shard_map(
        functools.partial(on_device, n_grp, n_row, 4),
        mesh=mesh,
        in_specs=in_specs,
        out_specs=out_specs,
        check_vma=False,
    )
```
